256 devices in a mesh: seq: 32 (over y, x, core), tp: 8 (over z).
Axes of the slice: x: 4, y: 4, z: 8, core: 2. Of those that a mesh axis runs over, the one named last changes fastest.
Arguments:
- hidden_in: bfloat16 [2, 16384, 2560], P(None, 'seq'), may hold values from -6 to 6
- gate_proj: bfloat16 [2560, 5120], P(None, 'tp'), may hold values from -0.125 to 0.125
- value_proj: bfloat16 [2560, 5120], P(None, 'tp'), may hold values from -0.125 to 0.125
- bc_proj: bfloat16 [2560, 256], P(None, 'tp'), may hold values from -0.125 to 0.125
- step_proj: bfloat16 [2560, 80], P(None, 'tp'), may hold values from -0.125 to 0.125
- value_conv: float32 [4, 5120], P(None, 'tp'), may hold values from -3 to 3
- bc_conv: float32 [4, 256], replicated, may hold values from -3 to 3
- step_bias: float32 [80], P('tp'), may hold values from -1.5 to 0
- log_rate: float32 [80], P('tp'), as said below
- norm_gain: float32 [5120], P('tp'), may hold values from 0.25 to 1.75
Outputs:
- mixer_out: bfloat16 [2, 16384, 5120], P(None, 'seq', 'tp')
The draws below stay inside these ranges and needn't reach their ends.
Inputs may be any that keep to these rules, and one draw needn't show every extreme that they name: log_rate lies between -1.5 - ln(16384) and 1.0 - ln(16384).
All inputs are finite; a program needn't handle non-finite values.
Results may differ from the reference program's by a relative error of at most 0.0095.
Values may be sent and summed in bfloat16 or wider, within the bound.
A program may use at most 128 MiB of HBM per device.

```python
import math
import jax
import jax.numpy as jnp
from jax import lax

D = 2560
DI = 5120
HEADS = 80
HEAD_DIM = 64
STATE = 128
CONV = 4
BATCH = 2
BLOCK = 64
SEQ_LEN = 16384


def draw_log_rate(key, part):
    shift = math.log(SEQ_LEN)
    return jax.random.uniform(key, (HEADS,), jnp.float32, -1.5 - shift, 1.0 - shift)


def level_of(own_key, dims, cuts, smallest, top_value):
    def one(axis_at, blocks):
        draws = jax.random.uniform(jax.random.fold_in(jax.random.fold_in(own_key, 6), axis_at), (blocks,), jnp.float32, smallest / len(cuts), top_value / len(cuts))
        return jnp.repeat(jnp.exp(draws), dims[axis_at] // blocks).reshape((-1,) + (1,) * (len(dims) - axis_at - 1))

    level = one(*cuts[0])
    for cut in cuts[1:]:
        level = level * one(*cut)
    return level


def noise(rng, extent, deviation, reach, shards=(), kind=jnp.bfloat16):
    entries = deviation * jax.random.normal(rng, extent, jnp.float32)
    if shards:
        entries = entries * level_of(rng, extent, shards, -0.22, 0.18)
    return jnp.clip(entries, -reach, reach).astype(kind)


def setup_inputs(seed: int = 0) -> dict:
    streams_of = jax.random.split(jax.random.key(seed), 11)
    hidden_in = noise(streams_of[0], (BATCH, SEQ_LEN, D), 1.0, 6.0, ((1, 32),))
    gate_proj = noise(streams_of[1], (D, DI), D ** -0.5, 0.125, ((1, 8),))
    value_proj = noise(streams_of[2], (D, DI), D ** -0.5, 0.125, ((1, 8),))
    bc_proj = noise(streams_of[3], (D, 2 * STATE), D ** -0.5, 0.125, ((1, 8),))
    step_proj = noise(streams_of[4], (D, HEADS), D ** -0.5, 0.125, ((1, 8),))
    value_conv = noise(streams_of[5], (CONV, DI), CONV ** -0.5, 3.0, ((1, 8),), jnp.float32)
    bc_conv = noise(streams_of[6], (CONV, 2 * STATE), CONV ** -0.5, 3.0, (), jnp.float32)
    step_bias = jnp.clip(-1.5 + 1.5 * jax.random.uniform(streams_of[7], (HEADS,), jnp.float32) ** level_of(streams_of[7], (HEADS,), ((0, 8),), -0.2, 0.2), -1.5, 0.0)
    log_rate = draw_log_rate(jax.random.fold_in(streams_of[10], 71), 0)
    norm_gain = jnp.clip(1.0 + 0.15 * jax.random.normal(streams_of[9], (DI,), jnp.float32), 0.25, 1.75)
    return {"hidden_in": hidden_in, "gate_proj": gate_proj, "value_proj": value_proj, "bc_proj": bc_proj, "step_proj": step_proj, "value_conv": value_conv, "bc_conv": bc_conv, "step_bias": step_bias, "log_rate": log_rate, "norm_gain": norm_gain}


epsilon = 1e-05

def conv_silu(padded, kernel, length):
    running = jnp.zeros((padded.shape[0], length, padded.shape[2]), jnp.float32)
    for tap_index in range(kernel.shape[0]):
        running = running + kernel[tap_index] * padded[:, tap_index:tap_index + length, :]
    return jax.nn.silu(running)

def block_step(carried, inputs):
    values, log_decay, step_sizes, b_rows, c_rows = inputs
    length = log_decay.shape[1]
    cumulative = jnp.cumsum(log_decay, axis=1)
    log_gap = cumulative[:, :, None, :] - cumulative[:, None, :, :]
    causal = jnp.arange(length)[:, None] >= jnp.arange(length)[None, :]
    weights_in = jnp.exp(jnp.where(causal[None, :, :, None], log_gap, -jnp.inf))
    scores = jnp.einsum('bin,bjn->bij', c_rows, b_rows, precision=lax.Precision.HIGHEST)
    mixing = scores[:, :, :, None] * weights_in * step_sizes[:, None, :, :]
    within = jnp.einsum('bijh,bjhp->bihp', mixing, values, precision=lax.Precision.HIGHEST)
    earlier = jnp.einsum('bin,bhpn->bihp', c_rows, carried, precision=lax.Precision.HIGHEST)
    earlier = earlier * jnp.exp(cumulative)[..., None]
    remain = jnp.exp(cumulative[:, -1:, :] - cumulative) * step_sizes
    added_state = jnp.einsum('bjh,bjhp,bjn->bhpn', remain, values, b_rows, precision=lax.Precision.HIGHEST)
    updated = jnp.exp(cumulative[:, -1, :])[:, :, None, None] * carried + added_state
    return (updated, within + earlier)

def to_blocks(series, batch_size, blocks):
    return jnp.moveaxis(series.reshape((batch_size, blocks, BLOCK) + series.shape[2:]), 1, 0)

def reference(hidden_in, gate_proj, value_proj, bc_proj, step_proj, value_conv, bc_conv, step_bias, log_rate, norm_gain):
    flat_rows = hidden_in.reshape(-1, D)
    gate_pre = jnp.dot(flat_rows, gate_proj, preferred_element_type=jnp.float32).astype(jnp.bfloat16)
    value_pre = jnp.dot(flat_rows, value_proj, preferred_element_type=jnp.float32).astype(jnp.bfloat16)
    bc_pre = jnp.dot(flat_rows, bc_proj, preferred_element_type=jnp.float32).astype(jnp.bfloat16)
    step_pre = jnp.dot(flat_rows, step_proj, preferred_element_type=jnp.float32)
    value_pad = jnp.pad(value_pre.reshape(BATCH, SEQ_LEN, DI).astype(jnp.float32), ((0, 0), (CONV - 1, 0), (0, 0)))
    bc_pad = jnp.pad(bc_pre.reshape(BATCH, SEQ_LEN, 2 * STATE).astype(jnp.float32), ((0, 0), (CONV - 1, 0), (0, 0)))
    values = conv_silu(value_pad, value_conv, SEQ_LEN).reshape(BATCH, SEQ_LEN, HEADS, HEAD_DIM)
    bc_rows = conv_silu(bc_pad, bc_conv, SEQ_LEN)
    b_rows = bc_rows[..., :STATE]
    c_rows = bc_rows[..., STATE:]
    step_sizes = jax.nn.softplus(step_pre.reshape(BATCH, SEQ_LEN, HEADS) + step_bias)
    log_decay = -step_sizes * jnp.exp(log_rate)
    blocks = SEQ_LEN // BLOCK
    initial = jnp.zeros((BATCH, HEADS, HEAD_DIM, STATE), jnp.float32)
    final_state, outputs = lax.scan(block_step, initial, (to_blocks(values, BATCH, blocks), to_blocks(log_decay, BATCH, blocks), to_blocks(step_sizes, BATCH, blocks), to_blocks(b_rows, BATCH, blocks), to_blocks(c_rows, BATCH, blocks)))
    mixed_out = jnp.moveaxis(outputs, 0, 1).reshape(BATCH, SEQ_LEN, DI)
    gated_out = mixed_out * jax.nn.silu(gate_pre.reshape(BATCH, SEQ_LEN, DI).astype(jnp.float32))
    scale_sq = lax.optimization_barrier(jnp.sum(gated_out * gated_out, axis=-1, keepdims=True)) / DI
    return (gated_out * lax.rsqrt(scale_sq + epsilon) * norm_gain).astype(jnp.bfloat16)
```

```python
import functools
import math

import jax
import jax.numpy as jnp
from jax import lax
from jax.experimental import pallas as pl
from jax.experimental.pallas import tpu as pltpu
from jax.sharding import PartitionSpec as P

MESH = pl.DeviceIdType.MESH
F32, BF16 = jnp.float32, jnp.bfloat16
HEAD_DIM = 64
STATE = 128
CONV = 4
HALO = 16
CHUNK = 128
EPSILON = 1e-05
NN = (((1,), (0,)), ((), ()))
TN = (((0,), (0,)), ((), ()))
NT = (((1,), (1,)), ((), ()))


def dot(a, b, dims=NN):
    return lax.dot_general(a, b, dims, preferred_element_type=F32)


def split2(x):
    high = x.astype(BF16)
    low = (x - high.astype(F32)).astype(BF16)
    return jnp.concatenate([high, low], axis=0)


def silu(x):
    return x * lax.logistic(x)


def conv_silu(window, taps, rows):
    total = taps[0:1] * window[5 : 5 + rows]
    for k in range(1, CONV):
        total = total + taps[k : k + 1] * window[5 + k : 5 + k + rows]
    return silu(total)


def kernel(
    n, nz, batch, length, inner, heads,
    hid_in, gate_in, value_in, bc_in, step_in, vconv, bconv, bias, rate, gain,
    out,
    hid, wcat, bcw, stw, wsm, small, pre, xp, lhs, tbuf, bct, bcall, dsend, dall, dexp,
    sbuf, rbuf, pbuf, qbuf, sssend, ssall, rowx, e1t, e2t,
    load_sem, halo_s, halo_r, bc_s, bc_r, d_s, d_r, p_s, p_r, q_s, q_r, ss_s, ss_r,
):
    me = lax.axis_index("seq")
    z = lax.axis_index("tp")
    step_rows = length + HALO
    chunks = length // CHUNK
    piece = batch * STATE // n
    per_batch = n // batch
    nbc = bct.shape[0]
    width = hid.shape[1]

    loads = []
    for b in range(batch):
        loads.append(
            pltpu.make_async_copy(
                hid_in.at[b], hid.at[pl.ds(b * step_rows + HALO, length)], load_sem.at[b]
            )
        )
    loads.append(pltpu.make_async_copy(bc_in, bcw, load_sem.at[2]))
    loads.append(pltpu.make_async_copy(step_in, stw, load_sem.at[3]))
    loads.append(pltpu.make_async_copy(value_in, wcat.at[:, pl.ds(0, inner)], load_sem.at[4]))
    loads.append(pltpu.make_async_copy(gate_in, wcat.at[:, pl.ds(inner, inner)], load_sem.at[5]))
    for k in (2, 3, 0, 1, 4, 5):
        loads[k].start()

    barrier = pltpu.get_barrier_semaphore()

    def greet_seq(d, carry):
        pl.semaphore_signal(
            barrier, inc=1, device_id={"seq": lax.rem(me + d, n)}, device_id_type=MESH
        )
        return carry

    def greet_tp(d, carry):
        pl.semaphore_signal(
            barrier, inc=1, device_id={"tp": lax.rem(z + d, nz)}, device_id_type=MESH
        )
        return carry

    lax.fori_loop(1, n, greet_seq, 0)
    lax.fori_loop(1, nz, greet_tp, 0)

    head_of = lax.broadcasted_iota(jnp.int32, (16, inner), 1) // HEAD_DIM
    spread16 = (head_of == lax.broadcasted_iota(jnp.int32, (16, inner), 0)).astype(F32)
    spread = jnp.concatenate([spread16, spread16], axis=0).astype(BF16)
    upper = (
        lax.broadcasted_iota(jnp.int32, (length, length), 0)
        <= lax.broadcasted_iota(jnp.int32, (length, length), 1)
    ).astype(F32).astype(BF16)

    pl.semaphore_wait(barrier, n - 1 + nz - 1)

    def halo_copy(b, target):
        return pltpu.make_async_remote_copy(
            src_ref=hid_in.at[b, pl.ds(length - HALO, HALO)],
            dst_ref=hid.at[pl.ds(b * step_rows, HALO)],
            send_sem=halo_s.at[b],
            recv_sem=halo_r.at[b],
            device_id={"seq": target},
            device_id_type=MESH,
        )

    following = lax.rem(me + 1, n)

    @pl.when(me < n - 1)
    def _():
        for b in range(batch):
            halo_copy(b, following).start()

    @pl.when(me == 0)
    def _():
        for b in range(batch):
            hid[pl.ds(b * step_rows, HALO), :] = jnp.zeros((HALO, width), BF16)

    loads[2].wait()
    loads[3].wait()
    wsm[:, 0:nbc] = bcw[...]
    wsm[:, 128 : 128 + heads] = stw[...]
    for b in range(batch):
        loads[b].wait()
        rows = pl.ds(b * step_rows + HALO, length)
        small[rows, :] = dot(hid[rows, :], wsm[...])

    @pl.when(me > 0)
    def _():
        for b in range(batch):
            halo_copy(b, following).wait_recv()

    edge = dot(
        jnp.concatenate([hid[pl.ds(b * step_rows, HALO), :] for b in range(batch)], axis=0),
        wsm[...],
    )
    for b in range(batch):
        small[pl.ds(b * step_rows, HALO), :] = edge[b * HALO : (b + 1) * HALO]

    taps = pltpu.roll(
        jnp.concatenate([bconv[...], jnp.zeros((8 - CONV, 2 * STATE), F32)], axis=0),
        lax.rem(2 * STATE - z * nbc, 2 * STATE),
        1,
    )[:, 0:128]
    for b in range(batch):
        base = b * step_rows
        window = small[pl.ds(base + 8, length + 8), 0:128].astype(BF16).astype(F32)
        rows = conv_silu(window, taps, length)
        bct[:, b * length : (b + 1) * length] = jnp.transpose(rows)[0:nbc].astype(BF16)
    bcall[z] = bct[...]

    def bc_copy(source, target):
        return pltpu.make_async_remote_copy(
            src_ref=bct,
            dst_ref=bcall.at[source],
            send_sem=bc_s.at[target],
            recv_sem=bc_r.at[source],
            device_id={"tp": target},
            device_id_type=MESH,
        )

    def bc_start(d, carry):
        bc_copy(z, lax.rem(z + d, nz)).start()
        return carry

    lax.fori_loop(1, nz, bc_start, 0)

    table = jnp.concatenate([bias[...], rate[...], jnp.zeros((6, heads), F32)], axis=0)
    table = jnp.concatenate([table, jnp.zeros((8, 128 - heads), F32)], axis=1)
    columns = jnp.transpose(table)
    bias_col, rate_col = columns[0:16, 0:1], jnp.exp(columns[0:16, 1:2])
    live = lax.broadcasted_iota(jnp.int32, (16, length), 0) < heads
    steps, parts = [], []
    for b in range(batch):
        raw = jnp.transpose(small[pl.ds(b * step_rows + HALO, length), 128:256])[0:16]
        raw = jnp.where(live, raw + bias_col, 0.0)
        size = jnp.maximum(raw, 0.0) + jnp.log1p(jnp.exp(-jnp.abs(raw)))
        size = jnp.where(live, size, 0.0)
        steps.append(size)
        parts.append(split2(-size * rate_col))
    summed = dot(jnp.concatenate(parts, axis=0), upper)
    lane = lax.broadcasted_iota(jnp.int32, (16, 128), 1)
    factors = jnp.zeros((16, 128), F32)
    for b in range(batch):
        cum = summed[32 * b : 32 * b + 16] + summed[32 * b + 16 : 32 * b + 32]
        begin = jnp.zeros((16, 1), F32)
        for c in range(chunks):
            here = cum[:, c * CHUNK : (c + 1) * CHUNK]
            end = here[:, CHUNK - 1 : CHUNK]
            ref = 0.5 * (begin + end)
            q = b * chunks + c
            e1t[q] = split2(jnp.exp(ref - here) * steps[b][:, c * CHUNK : (c + 1) * CHUNK])
            e2t[q] = split2(jnp.exp(here - ref))
            for kind, value in enumerate((ref - begin, end - begin, end - ref, ref)):
                factors = jnp.where(lane == kind * 8 + q, value, factors)
            begin = end
        factors = jnp.where(lane == 32 + b, begin, factors)
    factors = jnp.exp(factors)
    rowx[...] = dot(split2(factors), spread, TN)
    totals = jnp.transpose(factors)
    for b in range(batch):
        row = jnp.concatenate(
            [totals[32 + b : 33 + b], jnp.zeros((1, 112), F32)], axis=1
        )
        dsend[b] = jnp.broadcast_to(row, (8, 128))

    def d_copy(source, target):
        return pltpu.make_async_remote_copy(
            src_ref=dsend.at[target // per_batch],
            dst_ref=dall.at[source],
            send_sem=d_s.at[target],
            recv_sem=d_r.at[source],
            device_id={"seq": target},
            device_id_type=MESH,
        )

    def d_start(d, carry):
        d_copy(me, lax.rem(me + d, n)).start()
        return carry

    lax.fori_loop(1, n, d_start, 0)
    dall[me] = dsend[me // per_batch]

    loads[4].wait()
    loads[5].wait()

    def project(t, carry):
        columns_at = pl.ds(pl.multiple_of(t * 256, 256), 256)
        for half in range(batch):
            rows = pl.ds(half * step_rows, step_rows)
            pre[rows, columns_at] = (
                dot(hid[rows, :], wcat[:, columns_at]).astype(BF16).astype(F32)
            )
        return carry

    lax.fori_loop(0, 2 * inner // 256, project, 0)

    vtaps = vconv[...]

    def values_of(q, carry):
        base = pl.multiple_of((q // chunks) * step_rows + lax.rem(q, chunks) * CHUNK + 8, 8)
        rows = conv_silu(pre[pl.ds(base, CHUNK + 8), 0:inner], vtaps, CHUNK)
        xp[q] = (rows * dot(e1t[q], spread, TN)).astype(BF16)
        at = pl.ds(base + 8, CHUNK)
        pre[at, inner:] = silu(pre[at, inner:]) * dot(e2t[q], spread, TN)
        return carry

    lax.fori_loop(0, batch * chunks, values_of, 0)

    def bc_wait(d, carry):
        bc_copy(lax.rem(z + d, nz), z).wait_recv()
        return carry

    lax.fori_loop(1, nz, bc_wait, 0)
    half = nz // 2
    causal = (
        lax.broadcasted_iota(jnp.int32, (CHUNK, CHUNK), 0)
        >= lax.broadcasted_iota(jnp.int32, (CHUNK, CHUNK), 1)
    )
    for b in range(batch):
        state = jnp.zeros((STATE, inner), F32)
        for c in range(chunks):
            q = b * chunks + c
            lanes = slice(b * length + c * CHUNK, b * length + (c + 1) * CHUNK)
            rows = bcall[0:half, :, lanes].reshape(STATE, CHUNK)
            if c:
                tbuf[q] = state * rowx[q : q + 1]
                state = state * rowx[8 + q : 9 + q]
            else:
                tbuf[q] = jnp.zeros((STATE, inner), F32)
            state = state + rowx[16 + q : 17 + q] * dot(rows, xp[q])
        sbuf[b * per_batch : (b + 1) * per_batch] = state.reshape(
            per_batch, piece, inner
        ).astype(BF16)
    rbuf[me] = sbuf[me]

    def p_copy(source, target):
        return pltpu.make_async_remote_copy(
            src_ref=sbuf.at[target],
            dst_ref=rbuf.at[source],
            send_sem=p_s.at[target],
            recv_sem=p_r.at[source],
            device_id={"seq": target},
            device_id_type=MESH,
        )

    def p_start(d, carry):
        p_copy(me, lax.rem(me + d, n)).start()
        return carry

    lax.fori_loop(1, n, p_start, 0)

    def d_wait(d, carry):
        d_copy(lax.rem(me + d, n), me).wait_recv()
        return carry

    lax.fori_loop(1, n, d_wait, 0)
    decays = dall[...].reshape(n * 8, 128)[:, 0:16]
    high = decays.astype(BF16)
    low = (decays - high.astype(F32)).astype(BF16)
    dexp[...] = (dot(high, spread[0:16]) + dot(low, spread[0:16])).reshape(n, 8, inner)

    for q in range(batch * chunks):
        lanes = slice(q * CHUNK, (q + 1) * CHUNK)
        b_t = bcall[0:half, :, lanes].reshape(STATE, CHUNK)
        c_t = bcall[half:nz, :, lanes].reshape(STATE, CHUNK)
        scores = dot(c_t, b_t, TN)
        lhs[q, :, 0:CHUNK] = jnp.where(causal, scores, 0.0).astype(BF16)
        lhs[q, :, CHUNK:] = jnp.transpose(c_t.astype(F32)).astype(BF16)

    def scan_step(i, prefix):
        @pl.when(i != me)
        def _():
            p_copy(i, me).wait_recv()

        pbuf[i] = prefix.astype(BF16)
        return dexp[i, 0:1, :] * prefix + rbuf[i].astype(F32)

    lax.fori_loop(0, n, scan_step, jnp.zeros((piece, inner), F32))

    def q_copy(source, target):
        return pltpu.make_async_remote_copy(
            src_ref=pbuf.at[target],
            dst_ref=qbuf.at[source],
            send_sem=q_s.at[target],
            recv_sem=q_r.at[source],
            device_id={"seq": target},
            device_id_type=MESH,
        )

    def q_start(d, carry):
        q_copy(me, lax.rem(me + d, n)).start()
        return carry

    lax.fori_loop(1, n, q_start, 0)
    qbuf[me] = pbuf[me]

    def q_wait(d, carry):
        q_copy(lax.rem(me + d, n), me).wait_recv()
        return carry

    lax.fori_loop(1, n, q_wait, 0)

    ones = jnp.ones((8, inner), BF16)
    picked = lax.broadcasted_iota(jnp.int32, (8, CHUNK), 0)
    squares = jnp.zeros((8, CHUNK), F32)
    gains = gain[...]
    for b in range(batch):
        entering = qbuf[b * per_batch : (b + 1) * per_batch].astype(F32).reshape(STATE, inner)
        for c in range(chunks):
            q = b * chunks + c
            state = (tbuf[q] + entering * rowx[24 + q : 25 + q]).astype(BF16)
            at = pl.ds(b * step_rows + HALO + c * CHUNK, CHUNK)
            mixed = dot(lhs[q], jnp.concatenate([xp[q], state], axis=0))
            gated = mixed * pre[at, inner:]
            pre[at, 0:inner] = gated * gains
            sums = dot(ones, (gated * gated).astype(BF16), NT)
            squares = jnp.where(picked == q, sums, squares)
    sssend[...] = squares

    def ss_copy(source, target):
        return pltpu.make_async_remote_copy(
            src_ref=sssend,
            dst_ref=ssall.at[source],
            send_sem=ss_s.at[target],
            recv_sem=ss_r.at[source],
            device_id={"tp": target},
            device_id_type=MESH,
        )

    def ss_start(d, carry):
        ss_copy(z, lax.rem(z + d, nz)).start()
        return carry

    lax.fori_loop(1, nz, ss_start, 0)
    ssall[z] = squares

    def ss_wait(d, carry):
        ss_copy(lax.rem(z + d, nz), z).wait_recv()
        return carry

    lax.fori_loop(1, nz, ss_wait, 0)
    whole = ssall[0]
    for s in range(1, nz):
        whole = whole + ssall[s]
    factor = lax.rsqrt(whole / (inner * nz) + EPSILON)
    wide = jnp.ones((16, 128), BF16)
    for b in range(batch):
        for c in range(chunks):
            q = b * chunks + c
            mine = split2(jnp.where(picked == q, factor, 0.0))
            scale = dot(mine, wide, TN)
            at = pl.ds(b * step_rows + HALO + c * CHUNK, CHUNK)
            for col in range(0, inner, 128):
                out[b, c * CHUNK : (c + 1) * CHUNK, col : col + 128] = (
                    pre[at, col : col + 128] * scale
                ).astype(BF16)

    @pl.when(me < n - 1)
    def _():
        for b in range(batch):
            halo_copy(b, following).wait_send()

    def seq_sent(d, carry):
        other = lax.rem(me + d, n)
        d_copy(me, other).wait_send()
        p_copy(me, other).wait_send()
        q_copy(me, other).wait_send()
        return carry

    def tp_sent(d, carry):
        other = lax.rem(z + d, nz)
        bc_copy(z, other).wait_send()
        ss_copy(z, other).wait_send()
        return carry

    lax.fori_loop(1, n, seq_sent, 0)
    lax.fori_loop(1, nz, tp_sent, 0)


def on_device(
    n, nz, hidden_in, gate_proj, value_proj, bc_proj, step_proj,
    value_conv, bc_conv, step_bias, log_rate, norm_gain,
):
    batch, length, width = hidden_in.shape
    inner, heads, nbc = value_proj.shape[1], step_proj.shape[1], bc_proj.shape[1]
    chunks = batch * length // CHUNK
    rows = batch * (length + HALO)
    piece = batch * STATE // n
    hbm = pl.BlockSpec(memory_space=pl.ANY)
    vmem = pl.BlockSpec(memory_space=pltpu.VMEM)
    dma = pltpu.SemaphoreType.DMA
    return pl.pallas_call(
        functools.partial(kernel, n, nz, batch, length, inner, heads),
        out_shape=jax.ShapeDtypeStruct((batch, length, inner), BF16),
        in_specs=[hbm] * 5 + [vmem] * 5,
        out_specs=vmem,
        scratch_shapes=[
            pltpu.VMEM((rows, width), BF16),
            pltpu.VMEM((width, 2 * inner), BF16),
            pltpu.VMEM((width, nbc), BF16),
            pltpu.VMEM((width, heads), BF16),
            pltpu.VMEM((width, 256), BF16),
            pltpu.VMEM((rows, 256), F32),
            pltpu.VMEM((rows, 2 * inner), F32),
            pltpu.VMEM((chunks, CHUNK, inner), BF16),
            pltpu.VMEM((chunks, CHUNK, CHUNK + STATE), BF16),
            pltpu.VMEM((chunks, STATE, inner), F32),
            pltpu.VMEM((nbc, batch * length), BF16),
            pltpu.VMEM((nz, nbc, batch * length), BF16),
            pltpu.VMEM((batch, 8, 128), F32),
            pltpu.VMEM((n, 8, 128), F32),
            pltpu.VMEM((n, 8, inner), F32),
            pltpu.VMEM((n, piece, inner), BF16),
            pltpu.VMEM((n, piece, inner), BF16),
            pltpu.VMEM((n, piece, inner), BF16),
            pltpu.VMEM((n, piece, inner), BF16),
            pltpu.VMEM((8, CHUNK), F32),
            pltpu.VMEM((nz, 8, CHUNK), F32),
            pltpu.VMEM((128, inner), F32),
            pltpu.VMEM((chunks, 32, CHUNK), BF16),
            pltpu.VMEM((chunks, 32, CHUNK), BF16),
            dma((6,)),
            dma((batch,)), dma((batch,)),
            dma((nz,)), dma((nz,)),
            dma((n,)), dma((n,)),
            dma((n,)), dma((n,)),
            dma((n,)), dma((n,)),
            dma((nz,)), dma((nz,)),
        ],
        compiler_params=pltpu.CompilerParams(
            collective_id=0, has_side_effects=True, vmem_limit_bytes=60 * 1024 * 1024
        ),
    )(
        hidden_in, gate_proj, value_proj, bc_proj, step_proj, value_conv, bc_conv,
        step_bias.reshape(1, heads), log_rate.reshape(1, heads), norm_gain.reshape(1, inner),
    )


def solution(mesh):
    n, nz = mesh.shape["seq"], mesh.shape["tp"]
    return jax.shard_map(
        functools.partial(on_device, n, nz),
        mesh=mesh,
        in_specs=(
            P(None, "seq", None), P(None, "tp"), P(None, "tp"), P(None, "tp"), P(None, "tp"),
            P(None, "tp"), P(), P("tp"), P("tp"), P("tp"),
        ),
        out_specs=P(None, "seq", "tp"),
        check_vma=False,
    )
```

```python
import functools
import math

import jax
import jax.numpy as jnp
from jax import lax
from jax.experimental import pallas as pl
from jax.experimental.pallas import tpu as pltpu
from jax.sharding import PartitionSpec as P

MESH = pl.DeviceIdType.MESH
F32, BF16 = jnp.float32, jnp.bfloat16
HEAD_DIM = 64
STATE = 128
CONV = 4
HALO = 16
CHUNK = 128
EPSILON = 1e-05
NN = (((1,), (0,)), ((), ()))
TN = (((0,), (0,)), ((), ()))
NT = (((1,), (1,)), ((), ()))


def dot(a, b, dims=NN):
    return lax.dot_general(a, b, dims, preferred_element_type=F32)


def split2(x):
    high = x.astype(BF16)
    low = (x - high.astype(F32)).astype(BF16)
    return jnp.concatenate([high, low], axis=0)


def silu(x):
    half = 0.5 * x
    return half * jnp.tanh(half) + half


def conv_silu(window, taps, rows):
    total = taps[0:1] * window[5 : 5 + rows]
    for k in range(1, CONV):
        total = total + taps[k : k + 1] * window[5 + k : 5 + k + rows]
    return silu(total)


def kernel(
    n, nz, batch, length, inner, heads,
    hid_in, gate_in, value_in, bc_in, step_in, vconv_in, bconv_in, bias_in, rate_in, gain_in,
    out,
    vconv, bconv, bias, rate, gain, hid, wcat, stw, wsm, small, pre, xp, lhs, tbuf, bct, bcall, dsend, dall, dexp,
    sbuf, rbuf, pbuf, qbuf, sssend, ssall, rowx, e1t, e2t,
    load_sem, halo_s, halo_r, bc_s, bc_r, d_s, d_r, p_s, p_r, q_s, q_r, ss_s, ss_r,
):
    me = lax.axis_index("seq")
    z = lax.axis_index("tp")
    step_rows = length + HALO
    chunks = length // CHUNK
    piece = batch * STATE // n
    per_batch = n // batch
    nbc = bct.shape[0]
    width = hid.shape[1]

    loads = []
    for b in range(batch):
        loads.append(
            pltpu.make_async_copy(
                hid_in.at[b], hid.at[pl.ds(b * step_rows + HALO, length)], load_sem.at[b]
            )
        )
    loads.append(pltpu.make_async_copy(bc_in, wsm.at[pl.ds(0, nbc)], load_sem.at[2]))
    loads.append(pltpu.make_async_copy(step_in, stw, load_sem.at[3]))
    loads.append(pltpu.make_async_copy(value_in, wcat.at[:, pl.ds(0, inner)], load_sem.at[4]))
    loads.append(pltpu.make_async_copy(gate_in, wcat.at[:, pl.ds(inner, inner)], load_sem.at[5]))
    tables = ((vconv_in, vconv), (bconv_in, bconv), (bias_in, bias), (rate_in, rate), (gain_in, gain))
    for k, (source, target) in enumerate(tables):
        loads.append(pltpu.make_async_copy(source, target, load_sem.at[6 + k]))
    for k in (2, 3, 0, 1, 8, 9, 7, 6, 10, 4, 5):
        loads[k].start()

    barrier = pltpu.get_barrier_semaphore()

    def greet_seq(d, carry):
        pl.semaphore_signal(
            barrier, inc=1, device_id={"seq": lax.rem(me + d, n)}, device_id_type=MESH
        )
        return carry

    def greet_tp(d, carry):
        pl.semaphore_signal(
            barrier, inc=1, device_id={"tp": lax.rem(z + d, nz)}, device_id_type=MESH
        )
        return carry

    lax.fori_loop(1, n, greet_seq, 0)
    lax.fori_loop(1, nz, greet_tp, 0)

    head_of = lax.broadcasted_iota(jnp.int32, (16, inner), 1) // HEAD_DIM
    spread16 = (head_of == lax.broadcasted_iota(jnp.int32, (16, inner), 0)).astype(F32)
    spread = jnp.concatenate([spread16, spread16], axis=0).astype(BF16)
    upper = (
        lax.broadcasted_iota(jnp.int32, (length, length), 0)
        <= lax.broadcasted_iota(jnp.int32, (length, length), 1)
    ).astype(F32).astype(BF16)

    loads[2].wait()
    loads[3].wait()
    wsm[nbc : nbc + heads, :] = stw[...]
    wsm[nbc + heads : nbc + 16, :] = jnp.zeros((16 - heads, width), BF16)

    def project_small(b):
        loads[b].wait()
        rows = pl.ds(b * step_rows + HALO, length)
        small[rows, :] = dot(hid[rows, :], wsm[...], NT)

    project_small(0)
    pl.semaphore_wait(barrier, n - 1 + nz - 1)

    def halo_copy(b, target):
        return pltpu.make_async_remote_copy(
            src_ref=hid_in.at[b, pl.ds(length - HALO, HALO)],
            dst_ref=hid.at[pl.ds(b * step_rows, HALO)],
            send_sem=halo_s.at[b],
            recv_sem=halo_r.at[b],
            device_id={"seq": target},
            device_id_type=MESH,
        )

    following = lax.rem(me + 1, n)

    @pl.when(me < n - 1)
    def _():
        for b in range(batch):
            halo_copy(b, following).start()

    @pl.when(me == 0)
    def _():
        for b in range(batch):
            hid[pl.ds(b * step_rows, HALO), :] = jnp.zeros((HALO, width), BF16)

    for b in range(1, batch):
        project_small(b)

    loads[8].wait()
    loads[9].wait()
    table = jnp.concatenate([bias[...], rate[...], jnp.zeros((6, heads), F32)], axis=0)
    table = jnp.concatenate([table, jnp.zeros((8, 128 - heads), F32)], axis=1)
    columns = jnp.transpose(table)
    bias_col, rate_col = columns[0:16, 0:1], jnp.exp(columns[0:16, 1:2])
    live = lax.broadcasted_iota(jnp.int32, (16, length), 0) < heads
    steps, parts = [], []
    for b in range(batch):
        raw = jnp.transpose(small[pl.ds(b * step_rows + HALO, length), nbc : nbc + 16])
        raw = jnp.where(live, raw + bias_col, 0.0)
        size = jnp.maximum(raw, 0.0) + jnp.log1p(jnp.exp(-jnp.abs(raw)))
        size = jnp.where(live, size, 0.0)
        steps.append(size)
        parts.append(split2(-size * rate_col))
    summed = dot(jnp.concatenate(parts, axis=0), upper)
    lane = lax.broadcasted_iota(jnp.int32, (16, 128), 1)
    factors = jnp.zeros((16, 128), F32)
    for b in range(batch):
        cum = summed[32 * b : 32 * b + 16] + summed[32 * b + 16 : 32 * b + 32]
        begin = jnp.zeros((16, 1), F32)
        for c in range(chunks):
            here = cum[:, c * CHUNK : (c + 1) * CHUNK]
            end = here[:, CHUNK - 1 : CHUNK]
            ref = 0.5 * (begin + end)
            q = b * chunks + c
            e1t[q] = split2(jnp.exp(ref - here) * steps[b][:, c * CHUNK : (c + 1) * CHUNK])
            e2t[q] = split2(jnp.exp(here - ref))
            for kind, value in enumerate((ref - begin, end - begin, end - ref, ref)):
                factors = jnp.where(lane == kind * 8 + q, value, factors)
            begin = end
        factors = jnp.where(lane == 32 + b, begin, factors)
    factors = jnp.exp(factors)
    rowx[...] = dot(split2(factors), spread, TN)
    totals = jnp.transpose(factors)
    for b in range(batch):
        row = jnp.concatenate(
            [totals[32 + b : 33 + b], jnp.zeros((1, 112), F32)], axis=1
        )
        dsend[b] = jnp.broadcast_to(row, (8, 128))

    def d_copy(source, target):
        return pltpu.make_async_remote_copy(
            src_ref=dsend.at[target // per_batch],
            dst_ref=dall.at[source],
            send_sem=d_s.at[target],
            recv_sem=d_r.at[source],
            device_id={"seq": target},
            device_id_type=MESH,
        )

    def d_start(d, carry):
        d_copy(me, lax.rem(me + d, n)).start()
        return carry

    lax.fori_loop(1, n, d_start, 0)
    dall[me] = dsend[me // per_batch]

    @pl.when(me > 0)
    def _():
        for b in range(batch):
            halo_copy(b, following).wait_recv()

    edge = dot(
        jnp.concatenate([hid[pl.ds(b * step_rows, HALO), :] for b in range(batch)], axis=0),
        wsm[...],
        NT,
    )
    for b in range(batch):
        small[pl.ds(b * step_rows, HALO), :] = edge[b * HALO : (b + 1) * HALO]

    loads[7].wait()
    taps = pltpu.roll(
        jnp.concatenate([bconv[...], jnp.zeros((8 - CONV, 2 * STATE), F32)], axis=0),
        lax.rem(2 * STATE - z * nbc, 2 * STATE),
        1,
    )[:, 0:nbc]
    for b in range(batch):
        base = b * step_rows
        window = small[pl.ds(base + 8, length + 8), 0:nbc].astype(BF16).astype(F32)
        rows = conv_silu(window, taps, length)
        bct[:, b * length : (b + 1) * length] = jnp.transpose(rows).astype(BF16)
    bcall[z] = bct[...]

    def bc_copy(source, target):
        return pltpu.make_async_remote_copy(
            src_ref=bct,
            dst_ref=bcall.at[source],
            send_sem=bc_s.at[target],
            recv_sem=bc_r.at[source],
            device_id={"tp": target},
            device_id_type=MESH,
        )

    def bc_start(d, carry):
        bc_copy(z, lax.rem(z + d, nz)).start()
        return carry

    half = nz // 2
    lax.fori_loop(1, nz, bc_start, 0)

    loads[4].wait()
    loads[5].wait()

    def project(t, carry):
        columns_at = pl.ds(pl.multiple_of(t * 256, 256), 256)
        for half in range(batch):
            rows = pl.ds(half * step_rows, step_rows)
            pre[rows, columns_at] = (
                dot(hid[rows, :], wcat[:, columns_at]).astype(BF16).astype(F32)
            )
        return carry

    value_tiles = -(-inner // 256)
    lax.fori_loop(0, value_tiles, project, 0)

    loads[6].wait()
    vtaps = vconv[...]

    def values_of(q, carry):
        base = pl.multiple_of((q // chunks) * step_rows + lax.rem(q, chunks) * CHUNK + 8, 8)
        rows = conv_silu(pre[pl.ds(base, CHUNK + 8), 0:inner], vtaps, CHUNK)
        xp[q] = (rows * dot(e1t[q], spread, TN)).astype(BF16)
        return carry

    lax.fori_loop(0, batch * chunks, values_of, 0)

    lax.fori_loop(value_tiles, 2 * inner // 256, project, 0)

    def gates_of(q, carry):
        base = pl.multiple_of((q // chunks) * step_rows + lax.rem(q, chunks) * CHUNK + HALO, 8)
        at = pl.ds(base, CHUNK)
        pre[at, inner:] = silu(pre[at, inner:]) * dot(e2t[q], spread, TN)
        return carry

    lax.fori_loop(0, batch * chunks, gates_of, 0)

    def bc_wait(s, carry):
        @pl.when(s != z)
        def _():
            bc_copy(s, z).wait_recv()

        return carry

    lax.fori_loop(0, half, bc_wait, 0)

    causal = (
        lax.broadcasted_iota(jnp.int32, (CHUNK, CHUNK), 0)
        >= lax.broadcasted_iota(jnp.int32, (CHUNK, CHUNK), 1)
    )
    for b in range(batch):
        state = jnp.zeros((STATE, inner), F32)
        for c in range(chunks):
            q = b * chunks + c
            lanes = slice(b * length + c * CHUNK, b * length + (c + 1) * CHUNK)
            rows = bcall[0:half, :, lanes].reshape(STATE, CHUNK)
            if c:
                tbuf[q] = state * rowx[q : q + 1]
                state = state * rowx[8 + q : 9 + q]
            else:
                tbuf[q] = jnp.zeros((STATE, inner), F32)
            state = state + rowx[16 + q : 17 + q] * dot(rows, xp[q])
        sbuf[b * per_batch : (b + 1) * per_batch] = state.reshape(
            per_batch, piece, inner
        ).astype(BF16)
    rbuf[me] = sbuf[me]

    def p_copy(source, target):
        return pltpu.make_async_remote_copy(
            src_ref=sbuf.at[target],
            dst_ref=rbuf.at[source],
            send_sem=p_s.at[target],
            recv_sem=p_r.at[source],
            device_id={"seq": target},
            device_id_type=MESH,
        )

    def p_start(d, carry):
        p_copy(me, lax.rem(me + d, n)).start()
        return carry

    lax.fori_loop(1, n, p_start, 0)

    def d_wait(d, carry):
        d_copy(lax.rem(me + d, n), me).wait_recv()
        return carry

    lax.fori_loop(1, n, d_wait, 0)
    decays = dall[...].reshape(n * 8, 128)[:, 0:16]
    high = decays.astype(BF16)
    low = (decays - high.astype(F32)).astype(BF16)
    dexp[...] = (dot(high, spread[0:16]) + dot(low, spread[0:16])).reshape(n, 8, inner)

    def scan_step(i, prefix):
        @pl.when(i != me)
        def _():
            p_copy(i, me).wait_recv()

        pbuf[i] = prefix.astype(BF16)
        return dexp[i, 0:1, :] * prefix + rbuf[i].astype(F32)

    lax.fori_loop(0, n, scan_step, jnp.zeros((piece, inner), F32))

    def q_copy(source, target):
        return pltpu.make_async_remote_copy(
            src_ref=pbuf.at[target],
            dst_ref=qbuf.at[source],
            send_sem=q_s.at[target],
            recv_sem=q_r.at[source],
            device_id={"seq": target},
            device_id_type=MESH,
        )

    def q_start(d, carry):
        q_copy(me, lax.rem(me + d, n)).start()
        return carry

    lax.fori_loop(1, n, q_start, 0)
    qbuf[me] = pbuf[me]

    lax.fori_loop(half, nz, bc_wait, 0)
    for q in range(batch * chunks):
        lanes = slice(q * CHUNK, (q + 1) * CHUNK)
        b_t = bcall[0:half, :, lanes].reshape(STATE, CHUNK)
        c_t = bcall[half:nz, :, lanes].reshape(STATE, CHUNK)
        scores = dot(c_t, b_t, TN)
        lhs[q, :, 0:CHUNK] = jnp.where(causal, scores, 0.0).astype(BF16)
        lhs[q, :, CHUNK:] = jnp.transpose(c_t.astype(F32)).astype(BF16)

    def q_wait(d, carry):
        q_copy(lax.rem(me + d, n), me).wait_recv()
        return carry

    lax.fori_loop(1, n, q_wait, 0)

    ones = jnp.ones((8, inner), BF16)
    picked = lax.broadcasted_iota(jnp.int32, (8, CHUNK), 0)
    squares = jnp.zeros((8, CHUNK), F32)
    loads[10].wait()
    gains = gain[...].reshape(1, inner)
    for b in range(batch):
        entering = qbuf[b * per_batch : (b + 1) * per_batch].astype(F32).reshape(STATE, inner)
        for c in range(chunks):
            q = b * chunks + c
            state = (tbuf[q] + entering * rowx[24 + q : 25 + q]).astype(BF16)
            at = pl.ds(b * step_rows + HALO + c * CHUNK, CHUNK)
            mixed = dot(lhs[q], jnp.concatenate([xp[q], state], axis=0))
            gated = mixed * pre[at, inner:]
            pre[at, 0:inner] = gated * gains
            sums = dot(ones, (gated * gated).astype(BF16), NT)
            squares = jnp.where(picked == q, sums, squares)
    sssend[...] = squares

    def ss_copy(source, target):
        return pltpu.make_async_remote_copy(
            src_ref=sssend,
            dst_ref=ssall.at[source],
            send_sem=ss_s.at[target],
            recv_sem=ss_r.at[source],
            device_id={"tp": target},
            device_id_type=MESH,
        )

    def ss_start(d, carry):
        ss_copy(z, lax.rem(z + d, nz)).start()
        return carry

    lax.fori_loop(1, nz, ss_start, 0)
    ssall[z] = squares

    def ss_wait(d, carry):
        ss_copy(lax.rem(z + d, nz), z).wait_recv()
        return carry

    lax.fori_loop(1, nz, ss_wait, 0)
    whole = ssall[0]
    for s in range(1, nz):
        whole = whole + ssall[s]
    factor = lax.rsqrt(whole / (inner * nz) + EPSILON)
    wide = jnp.ones((16, 128), BF16)
    for b in range(batch):
        for c in range(chunks):
            q = b * chunks + c
            mine = split2(jnp.where(picked == q, factor, 0.0))
            scale = dot(mine, wide, TN)
            at = pl.ds(b * step_rows + HALO + c * CHUNK, CHUNK)
            for col in range(0, inner, 128):
                out[b, c * CHUNK : (c + 1) * CHUNK, col : col + 128] = (
                    pre[at, col : col + 128] * scale
                ).astype(BF16)

    @pl.when(me < n - 1)
    def _():
        for b in range(batch):
            halo_copy(b, following).wait_send()

    def seq_sent(d, carry):
        other = lax.rem(me + d, n)
        d_copy(me, other).wait_send()
        p_copy(me, other).wait_send()
        q_copy(me, other).wait_send()
        return carry

    def tp_sent(d, carry):
        other = lax.rem(z + d, nz)
        bc_copy(z, other).wait_send()
        ss_copy(z, other).wait_send()
        return carry

    lax.fori_loop(1, n, seq_sent, 0)
    lax.fori_loop(1, nz, tp_sent, 0)


def on_device(
    n, nz, hidden_in, gate_proj, value_proj, bc_proj, step_proj,
    value_conv, bc_conv, step_bias, log_rate, norm_gain,
):
    batch, length, width = hidden_in.shape
    inner, heads, nbc = value_proj.shape[1], step_proj.shape[1], bc_proj.shape[1]
    chunks = batch * length // CHUNK
    rows = batch * (length + HALO)
    piece = batch * STATE // n
    hbm = pl.BlockSpec(memory_space=pltpu.HBM)
    vmem = pl.BlockSpec(memory_space=pltpu.VMEM)
    dma = pltpu.SemaphoreType.DMA
    return pl.pallas_call(
        functools.partial(kernel, n, nz, batch, length, inner, heads),
        out_shape=jax.ShapeDtypeStruct((batch, length, inner), BF16),
        in_specs=[hbm] * 10,
        out_specs=vmem,
        scratch_shapes=[
            pltpu.VMEM(value_conv.shape, F32),
            pltpu.VMEM(bc_conv.shape, F32),
            pltpu.VMEM((1, heads), F32),
            pltpu.VMEM((1, heads), F32),
            pltpu.VMEM((inner,), F32),
            pltpu.VMEM((rows, width), BF16),
            pltpu.VMEM((width, 2 * inner), BF16),
            pltpu.VMEM((heads, width), BF16),
            pltpu.VMEM((nbc + 16, width), BF16),
            pltpu.VMEM((rows, nbc + 16), F32),
            pltpu.VMEM((rows, 2 * inner), F32),
            pltpu.VMEM((chunks, CHUNK, inner), BF16),
            pltpu.VMEM((chunks, CHUNK, CHUNK + STATE), BF16),
            pltpu.VMEM((chunks, STATE, inner), F32),
            pltpu.VMEM((nbc, batch * length), BF16),
            pltpu.VMEM((nz, nbc, batch * length), BF16),
            pltpu.VMEM((batch, 8, 128), F32),
            pltpu.VMEM((n, 8, 128), F32),
            pltpu.VMEM((n, 8, inner), F32),
            pltpu.VMEM((n, piece, inner), BF16),
            pltpu.VMEM((n, piece, inner), BF16),
            pltpu.VMEM((n, piece, inner), BF16),
            pltpu.VMEM((n, piece, inner), BF16),
            pltpu.VMEM((8, CHUNK), F32),
            pltpu.VMEM((nz, 8, CHUNK), F32),
            pltpu.VMEM((128, inner), F32),
            pltpu.VMEM((chunks, 32, CHUNK), BF16),
            pltpu.VMEM((chunks, 32, CHUNK), BF16),
            dma((11,)),
            dma((batch,)), dma((batch,)),
            dma((nz,)), dma((nz,)),
            dma((n,)), dma((n,)),
            dma((n,)), dma((n,)),
            dma((n,)), dma((n,)),
            dma((nz,)), dma((nz,)),
        ],
        compiler_params=pltpu.CompilerParams(
            collective_id=0, has_side_effects=True, vmem_limit_bytes=52 * 1024 * 1024
        ),
    )(
        *(
            pltpu.with_memory_space_constraint(x, pltpu.HBM)
            for x in (
                hidden_in, gate_proj, value_proj, bc_proj.T, step_proj.T, value_conv, bc_conv,
                step_bias.reshape(1, heads), log_rate.reshape(1, heads), norm_gain,
            )
        )
    )


def solution(mesh):
    n, nz = mesh.shape["seq"], mesh.shape["tp"]
    return jax.shard_map(
        functools.partial(on_device, n, nz),
        mesh=mesh,
        in_specs=(
            P(None, "seq", None), P(None, "tp"), P(None, "tp"), P(None, "tp"), P(None, "tp"),
            P(None, "tp"), P(), P("tp"), P("tp"), P("tp"),
        ),
        out_specs=P(None, "seq", "tp"),
        check_vma=False,
    )
```

```python
import functools
import math

import jax
import jax.numpy as jnp
from jax import lax
from jax.experimental import pallas as pl
from jax.experimental.pallas import tpu as pltpu
from jax.sharding import PartitionSpec as P

MESH = pl.DeviceIdType.MESH
F32, BF16 = jnp.float32, jnp.bfloat16
HEAD_DIM = 64
STATE = 128
CONV = 4
EARLY_GATE = True
HALO = 16
CHUNK = 128
EPSILON = 1e-05
NN = (((1,), (0,)), ((), ()))
TN = (((0,), (0,)), ((), ()))
NT = (((1,), (1,)), ((), ()))


def dot(a, b, dims=NN):
    return lax.dot_general(a, b, dims, preferred_element_type=F32)


def split2(x):
    high = x.astype(BF16)
    low = (x - high.astype(F32)).astype(BF16)
    return jnp.concatenate([high, low], axis=0)


def bulk(view, send_sem, recv_sem, device_id):
    return pltpu.make_async_remote_copy(
        src_ref=view,
        dst_ref=view,
        send_sem=send_sem,
        recv_sem=recv_sem,
        device_id=device_id,
        device_id_type=MESH,
    )


def silu(x):
    half = 0.5 * x
    return half * jnp.tanh(half) + half


def conv_silu(window, taps, rows):
    total = taps[0:1] * window[5 : 5 + rows]
    for k in range(1, CONV):
        total = total + taps[k : k + 1] * window[5 + k : 5 + k + rows]
    return silu(total)


def kernel(
    n, nz, batch, length, inner, heads,
    hid_in, gate_in, value_in, bc_in, step_in, vconv_in, bconv_in, bias_in, rate_in, gain_in,
    out,
    vconv, bconv, bias, rate, gain, hid, wcat, stw, wsm, pre, xp, lhs, tbuf, bct, bcall, edget, edgeall, brows, crows, dsend, dall, dexp,
    sbuf, rbuf, pbuf, qbuf, sssend, ssall, rowx, e1t, e2t,
    load_sem, halo_s, halo_r, bc_s, bc_r, edge_s, edge_r, d_s, d_r, p_s, p_r, q_s, q_r, ss_s, ss_r,
):
    me = lax.axis_index("seq")
    z = lax.axis_index("tp")
    step_rows = length + HALO
    chunks = length // CHUNK
    piece = batch * STATE // n
    per_batch = n // batch
    nbc = bct.shape[1]
    half = nz // 2
    next_seq, next_tp = {"seq": lax.rem(me + 1, n)}, {"tp": lax.rem(z + 1, nz)}
    width = hid.shape[1]

    loads = []
    for b in range(batch):
        loads.append(
            pltpu.make_async_copy(
                hid_in.at[b], hid.at[pl.ds(b * step_rows + HALO, length)], load_sem.at[b]
            )
        )
    loads.append(pltpu.make_async_copy(bc_in, wsm.at[pl.ds(0, nbc)], load_sem.at[2]))
    loads.append(pltpu.make_async_copy(step_in, stw, load_sem.at[3]))
    loads.append(pltpu.make_async_copy(value_in, wcat.at[:, pl.ds(0, inner)], load_sem.at[4]))
    loads.append(pltpu.make_async_copy(gate_in, wcat.at[:, pl.ds(inner, inner)], load_sem.at[5]))
    tables = ((vconv_in, vconv), (bconv_in, bconv), (bias_in, bias), (rate_in, rate), (gain_in, gain))
    for k, (source, target) in enumerate(tables):
        loads.append(pltpu.make_async_copy(source, target, load_sem.at[6 + k]))
    for k in (2, 3, 0, 1, 8, 9, 7, 6, 10, 4, 5):
        loads[k].start()

    barrier = pltpu.get_barrier_semaphore()

    def greet_seq(d, carry):
        pl.semaphore_signal(
            barrier, inc=1, device_id={"seq": lax.rem(me + d, n)}, device_id_type=MESH
        )
        return carry

    def greet_tp(d, carry):
        pl.semaphore_signal(
            barrier, inc=1, device_id={"tp": lax.rem(z + d, nz)}, device_id_type=MESH
        )
        return carry

    lax.fori_loop(1, n, greet_seq, 0)
    lax.fori_loop(1, nz, greet_tp, 0)

    head_of = lax.broadcasted_iota(jnp.int32, (16, inner), 1) // HEAD_DIM
    spread16 = (head_of == lax.broadcasted_iota(jnp.int32, (16, inner), 0)).astype(F32)
    spread = jnp.concatenate([spread16, spread16], axis=0).astype(BF16)
    upper = (
        lax.broadcasted_iota(jnp.int32, (length, length), 0)
        <= lax.broadcasted_iota(jnp.int32, (length, length), 1)
    ).astype(F32).astype(BF16)

    loads[2].wait()
    loads[3].wait()
    wsm[nbc : nbc + heads, :] = stw[...]
    wsm[nbc + heads : nbc + 16, :] = jnp.zeros((16 - heads, width), BF16)

    raws = []

    def project_small(b):
        loads[b].wait()
        rows = pl.ds(b * step_rows + HALO, length)
        both = jnp.transpose(dot(hid[rows, :], wsm[...], NT))
        bct[b] = both[0:nbc].astype(BF16)
        raws.append(both[nbc : nbc + 16])

    project_small(0)
    pl.semaphore_wait(barrier, n - 1 + nz - 1)

    def halo_copy(b, target):
        return pltpu.make_async_remote_copy(
            src_ref=hid_in.at[b, pl.ds(length - HALO, HALO)],
            dst_ref=hid.at[pl.ds(b * step_rows, HALO)],
            send_sem=halo_s.at[b],
            recv_sem=halo_r.at[b],
            device_id={"seq": target},
            device_id_type=MESH,
        )

    following = lax.rem(me + 1, n)

    @pl.when(me < n - 1)
    def _():
        for b in range(batch):
            halo_copy(b, following).start()

    @pl.when(me == 0)
    def _():
        for b in range(batch):
            hid[pl.ds(b * step_rows, HALO), :] = jnp.zeros((HALO, width), BF16)

    def bc_copy(source, target, b):
        return pltpu.make_async_remote_copy(
            src_ref=bct.at[b],
            dst_ref=bcall.at[source, b],
            send_sem=bc_s,
            recv_sem=bc_r.at[source // half],
            device_id={"tp": target},
            device_id_type=MESH,
        )

    def send_bc(b):
        def bc_start(d, carry):
            bc_copy(z, lax.rem(z + d, nz), b).start()
            return carry

        lax.fori_loop(1, nz, bc_start, 0)
        bcall[z, b] = bct[b]

    send_bc(0)

    for b in range(1, batch):
        project_small(b)
        send_bc(b)

    loads[8].wait()
    loads[9].wait()
    table = jnp.concatenate([bias[...], rate[...], jnp.zeros((6, heads), F32)], axis=0)
    table = jnp.concatenate([table, jnp.zeros((8, 128 - heads), F32)], axis=1)
    columns = jnp.transpose(table)
    bias_col, rate_col = columns[0:16, 0:1], jnp.exp(columns[0:16, 1:2])
    live = lax.broadcasted_iota(jnp.int32, (16, length), 0) < heads
    steps, parts = [], []
    for b in range(batch):
        raw = jnp.where(live, raws[b] + bias_col, 0.0)
        size = jnp.maximum(raw, 0.0) + jnp.log1p(jnp.exp(-jnp.abs(raw)))
        size = jnp.where(live, size, 0.0)
        steps.append(size)
        parts.append(split2(-size * rate_col))
    summed = dot(jnp.concatenate(parts, axis=0), upper)
    lane = lax.broadcasted_iota(jnp.int32, (16, 128), 1)
    factors = jnp.zeros((16, 128), F32)
    for b in range(batch):
        cum = summed[32 * b : 32 * b + 16] + summed[32 * b + 16 : 32 * b + 32]
        begin = jnp.zeros((16, 1), F32)
        for c in range(chunks):
            here = cum[:, c * CHUNK : (c + 1) * CHUNK]
            end = here[:, CHUNK - 1 : CHUNK]
            ref = 0.5 * (begin + end)
            q = b * chunks + c
            e1t[q] = split2(jnp.exp(ref - here) * steps[b][:, c * CHUNK : (c + 1) * CHUNK])
            e2t[q] = split2(jnp.exp(here - ref))
            for kind, value in enumerate((ref - begin, end - begin, end - ref, ref)):
                factors = jnp.where(lane == kind * 8 + q, value, factors)
            begin = end
        factors = jnp.where(lane == 32 + b, begin, factors)
    factors = jnp.exp(factors)
    rowx[...] = dot(split2(factors), spread, TN)
    totals = jnp.transpose(factors)
    for b in range(batch):
        row = jnp.concatenate(
            [totals[32 + b : 33 + b], jnp.zeros((1, 112), F32)], axis=1
        )
        dsend[b] = jnp.broadcast_to(row, (8, 128))

    def d_copy(source, target):
        return pltpu.make_async_remote_copy(
            src_ref=dsend.at[target // per_batch],
            dst_ref=dall.at[source],
            send_sem=d_s,
            recv_sem=d_r,
            device_id={"seq": target},
            device_id_type=MESH,
        )

    def d_start(d, carry):
        d_copy(me, lax.rem(me + d, n)).start()
        return carry

    lax.fori_loop(1, n, d_start, 0)
    dall[me] = dsend[me // per_batch]

    loads[5].wait()
    tiles = 2 * inner // 256
    value_tiles = -(-inner // 256)

    def project_gate(t, carry):
        columns_at = pl.ds(pl.multiple_of(t * 256, 256), 256)
        for b in range(batch):
            rows = pl.ds(b * step_rows + HALO, length)
            pre[rows, columns_at] = dot(hid[rows, :], wcat[:, columns_at])
        return carry

    if EARLY_GATE:
        project_gate(tiles - 1, 0)

    @pl.when(me > 0)
    def _():
        for b in range(batch):
            halo_copy(b, following).wait_recv()

    edge = dot(
        wsm[0:nbc, :],
        jnp.concatenate([hid[pl.ds(b * step_rows, HALO), :] for b in range(batch)], axis=0),
        NT,
    )
    edge = jnp.concatenate([edge, jnp.zeros((nbc, 128 - batch * HALO), F32)], axis=1)
    edget[...] = edge.astype(BF16)
    edgeall[z] = edge.astype(BF16)

    def edge_copy(source, target):
        return pltpu.make_async_remote_copy(
            src_ref=edget,
            dst_ref=edgeall.at[source],
            send_sem=edge_s,
            recv_sem=edge_r,
            device_id={"tp": target},
            device_id_type=MESH,
        )

    def edge_start(d, carry):
        edge_copy(z, lax.rem(z + d, nz)).start()
        return carry

    lax.fori_loop(1, nz, edge_start, 0)

    loads[4].wait()

    def project(t, carry):
        columns_at = pl.ds(pl.multiple_of(t * 256, 256), 256)
        for half in range(batch):
            rows = pl.ds(half * step_rows, step_rows)
            pre[rows, columns_at] = (
                dot(hid[rows, :], wcat[:, columns_at]).astype(BF16).astype(F32)
            )
        return carry

    lax.fori_loop(0, value_tiles, project, 0)

    loads[6].wait()
    vtaps = vconv[...]

    def values_of(q, carry):
        base = pl.multiple_of((q // chunks) * step_rows + lax.rem(q, chunks) * CHUNK + 8, 8)
        rows = conv_silu(pre[pl.ds(base, CHUNK + 8), 0:inner], vtaps, CHUNK)
        xp[q] = (rows * dot(e1t[q], spread, TN)).astype(BF16)
        return carry

    lax.fori_loop(0, batch * chunks, values_of, 0)

    def bc_wait(group):
        blocks = [(z // half != group, half)]
        if half > 1:
            blocks.append((z // half == group, half - 1))
        for condition, count in blocks:

            @pl.when(condition)
            def _(count=count):
                bulk(bcall.at[pl.ds(0, count)], bc_s, bc_r.at[group], next_tp).wait_recv()

    loads[7].wait()
    taps = jnp.transpose(
        jnp.concatenate([bconv[...], jnp.zeros((8 - CONV, 2 * STATE), F32)], axis=0)
    )

    def conv_rows(first, b):
        sources = slice(first * half, (first + 1) * half)
        tail = edgeall[sources].reshape(STATE, 128).astype(F32)
        tail = pltpu.roll(tail, 128 - (b + 1) * HALO, 1)
        body = bcall[sources, b].reshape(STATE, length).astype(F32)
        whole = jnp.concatenate([tail, body], axis=1)
        weights = taps[first * STATE : (first + 1) * STATE]
        total = weights[:, CONV - 1 : CONV] * body
        for k in range(CONV - 1):
            shifted = pltpu.roll(whole, CONV - 1 - k, 1)[:, 128:]
            total = total + weights[:, k : k + 1] * shifted
        return silu(total).astype(BF16)

    bc_wait(0)
    bulk(edgeall.at[pl.ds(0, nz - 1)], edge_s, edge_r, next_tp).wait_recv()

    for b in range(batch):
        brows[:, b * length : (b + 1) * length] = conv_rows(0, b)

    causal = (
        lax.broadcasted_iota(jnp.int32, (CHUNK, CHUNK), 0)
        >= lax.broadcasted_iota(jnp.int32, (CHUNK, CHUNK), 1)
    )
    for b in range(batch):
        state = jnp.zeros((STATE, inner), F32)
        for c in range(chunks):
            q = b * chunks + c
            lanes = slice(b * length + c * CHUNK, b * length + (c + 1) * CHUNK)
            rows = brows[:, lanes]
            if c:
                tbuf[q] = state * rowx[q : q + 1]
                state = state * rowx[8 + q : 9 + q]
            else:
                tbuf[q] = jnp.zeros((STATE, inner), F32)
            state = state + rowx[16 + q : 17 + q] * dot(rows, xp[q])
        sbuf[b * per_batch : (b + 1) * per_batch] = state.reshape(
            per_batch, piece, inner
        ).astype(BF16)
    rbuf[me] = sbuf[me]

    def p_copy(source, target):
        return pltpu.make_async_remote_copy(
            src_ref=sbuf.at[target],
            dst_ref=rbuf.at[source],
            send_sem=p_s,
            recv_sem=p_r,
            device_id={"seq": target},
            device_id_type=MESH,
        )

    def p_start(d, carry):
        p_copy(me, lax.rem(me + d, n)).start()
        return carry

    lax.fori_loop(1, n, p_start, 0)

    lax.fori_loop(value_tiles, tiles - 1 if EARLY_GATE else tiles, project_gate, 0)

    def gates_of(q, carry):
        base = pl.multiple_of((q // chunks) * step_rows + lax.rem(q, chunks) * CHUNK + HALO, 8)
        at = pl.ds(base, CHUNK)
        pre[at, inner:] = silu(pre[at, inner:]) * dot(e2t[q], spread, TN)
        return carry

    lax.fori_loop(0, batch * chunks, gates_of, 0)

    bulk(dall.at[pl.ds(0, n - 1)], d_s, d_r, next_seq).wait_recv()
    decays = dall[...].reshape(n * 8, 128)[:, 0:16]
    high = decays.astype(BF16)
    low = (decays - high.astype(F32)).astype(BF16)
    dexp[...] = (dot(high, spread[0:16]) + dot(low, spread[0:16])).reshape(n, 8, inner)

    bc_wait(1)
    for b in range(batch):
        crows[:, b * length : (b + 1) * length] = conv_rows(1, b)
    for q in range(batch * chunks):
        lanes = slice(q * CHUNK, (q + 1) * CHUNK)
        b_t = brows[:, lanes]
        c_t = crows[:, lanes]
        scores = dot(c_t, b_t, TN)
        lhs[q, :, 0:CHUNK] = jnp.where(causal, scores, 0.0).astype(BF16)
        lhs[q, :, CHUNK:] = jnp.transpose(c_t.astype(F32)).astype(BF16)

    bulk(rbuf.at[pl.ds(0, n - 1)], p_s, p_r, next_seq).wait_recv()

    def scan_step(i, prefix):
        pbuf[i] = prefix.astype(BF16)
        return dexp[i, 0:1, :] * prefix + rbuf[i].astype(F32)

    lax.fori_loop(0, n, scan_step, jnp.zeros((piece, inner), F32))

    def q_copy(source, target):
        return pltpu.make_async_remote_copy(
            src_ref=pbuf.at[target],
            dst_ref=qbuf.at[source],
            send_sem=q_s,
            recv_sem=q_r,
            device_id={"seq": target},
            device_id_type=MESH,
        )

    def q_start(d, carry):
        q_copy(me, lax.rem(me + d, n)).start()
        return carry

    lax.fori_loop(1, n, q_start, 0)
    qbuf[me] = pbuf[me]

    bulk(dall.at[pl.ds(0, n - 1)], d_s, d_r, next_seq).wait_send()
    bulk(rbuf.at[pl.ds(0, n - 1)], p_s, p_r, next_seq).wait_send()

    bulk(qbuf.at[pl.ds(0, n - 1)], q_s, q_r, next_seq).wait_recv()

    ones = jnp.ones((8, inner), BF16)
    picked = lax.broadcasted_iota(jnp.int32, (8, CHUNK), 0)
    squares = jnp.zeros((8, CHUNK), F32)
    loads[10].wait()
    gains = gain[...].reshape(1, inner)
    for b in range(batch):
        entering = qbuf[b * per_batch : (b + 1) * per_batch].astype(F32).reshape(STATE, inner)
        for c in range(chunks):
            q = b * chunks + c
            state = (tbuf[q] + entering * rowx[24 + q : 25 + q]).astype(BF16)
            at = pl.ds(b * step_rows + HALO + c * CHUNK, CHUNK)
            mixed = dot(lhs[q], jnp.concatenate([xp[q], state], axis=0))
            gated = mixed * pre[at, inner:]
            pre[at, 0:inner] = gated * gains
            sums = dot(ones, (gated * gated).astype(BF16), NT)
            squares = jnp.where(picked == q, sums, squares)
    sssend[...] = squares

    def ss_copy(source, target):
        return pltpu.make_async_remote_copy(
            src_ref=sssend,
            dst_ref=ssall.at[source],
            send_sem=ss_s,
            recv_sem=ss_r,
            device_id={"tp": target},
            device_id_type=MESH,
        )

    def ss_start(d, carry):
        ss_copy(z, lax.rem(z + d, nz)).start()
        return carry

    lax.fori_loop(1, nz, ss_start, 0)
    ssall[z] = squares

    @pl.when(me < n - 1)
    def _():
        for b in range(batch):
            halo_copy(b, following).wait_send()

    bulk(qbuf.at[pl.ds(0, n - 1)], q_s, q_r, next_seq).wait_send()
    bulk(bcall.at[pl.ds(0, nz - 1)], bc_s, bc_r.at[0], next_tp).wait_send()
    bulk(edgeall.at[pl.ds(0, nz - 1)], edge_s, edge_r, next_tp).wait_send()

    bulk(ssall.at[pl.ds(0, nz - 1)], ss_s, ss_r, next_tp).wait_recv()

    whole = ssall[0]
    for s in range(1, nz):
        whole = whole + ssall[s]
    factor = lax.rsqrt(whole / (inner * nz) + EPSILON)
    wide = jnp.ones((16, 128), BF16)

    for b in range(batch):
        for c in range(chunks):
            q = b * chunks + c
            mine = split2(jnp.where(picked == q, factor, 0.0))
            scale = dot(mine, wide, TN)
            at = pl.ds(b * step_rows + HALO + c * CHUNK, CHUNK)
            for col in range(0, inner, 128):
                out[b, c * CHUNK : (c + 1) * CHUNK, col : col + 128] = (
                    pre[at, col : col + 128] * scale
                ).astype(BF16)

    bulk(ssall.at[pl.ds(0, nz - 1)], ss_s, ss_r, next_tp).wait_send()


def on_device(
    n, nz, hidden_in, gate_proj, value_proj, bc_proj, step_proj,
    value_conv, bc_conv, step_bias, log_rate, norm_gain,
):
    batch, length, width = hidden_in.shape
    inner, heads, nbc = value_proj.shape[1], step_proj.shape[1], bc_proj.shape[1]
    chunks = batch * length // CHUNK
    rows = batch * (length + HALO)
    piece = batch * STATE // n
    hbm = pl.BlockSpec(memory_space=pltpu.HBM)
    dma = pltpu.SemaphoreType.DMA
    return pl.pallas_call(
        functools.partial(kernel, n, nz, batch, length, inner, heads),
        out_shape=jax.ShapeDtypeStruct((batch, length, inner), BF16),
        in_specs=[hbm] * 10,
        out_specs=pl.BlockSpec(memory_space=pltpu.VMEM),
        scratch_shapes=[
            pltpu.VMEM(value_conv.shape, F32),
            pltpu.VMEM(bc_conv.shape, F32),
            pltpu.VMEM((1, heads), F32),
            pltpu.VMEM((1, heads), F32),
            pltpu.VMEM((inner,), F32),
            pltpu.VMEM((rows, width), BF16),
            pltpu.VMEM((width, 2 * inner), BF16),
            pltpu.VMEM((heads, width), BF16),
            pltpu.VMEM((nbc + 16, width), BF16),
            pltpu.VMEM((rows, 2 * inner), F32),
            pltpu.VMEM((chunks, CHUNK, inner), BF16),
            pltpu.VMEM((chunks, CHUNK, CHUNK + STATE), BF16),
            pltpu.VMEM((chunks, STATE, inner), F32),
            pltpu.VMEM((batch, nbc, length), BF16),
            pltpu.VMEM((nz, batch, nbc, length), BF16),
            pltpu.VMEM((nbc, 128), BF16),
            pltpu.VMEM((nz, nbc, 128), BF16),
            pltpu.VMEM((STATE, batch * length), BF16),
            pltpu.VMEM((STATE, batch * length), BF16),
            pltpu.VMEM((batch, 8, 128), F32),
            pltpu.VMEM((n, 8, 128), F32),
            pltpu.VMEM((n, 8, inner), F32),
            pltpu.VMEM((n, piece, inner), BF16),
            pltpu.VMEM((n, piece, inner), BF16),
            pltpu.VMEM((n, piece, inner), BF16),
            pltpu.VMEM((n, piece, inner), BF16),
            pltpu.VMEM((8, CHUNK), F32),
            pltpu.VMEM((nz, 8, CHUNK), F32),
            pltpu.VMEM((128, inner), F32),
            pltpu.VMEM((chunks, 32, CHUNK), BF16),
            pltpu.VMEM((chunks, 32, CHUNK), BF16),
            dma((11,)),
            dma((batch,)), dma((batch,)),
            dma, dma((2,)),
            dma, dma,
            dma, dma,
            dma, dma,
            dma, dma,
            dma, dma,
        ],
        compiler_params=pltpu.CompilerParams(
            collective_id=0, has_side_effects=True, vmem_limit_bytes=52 * 1024 * 1024
        ),
    )(
        *(
            pltpu.with_memory_space_constraint(x, pltpu.HBM)
            for x in (
                hidden_in, gate_proj, value_proj, bc_proj.T, step_proj.T, value_conv, bc_conv,
                step_bias.reshape(1, heads), log_rate.reshape(1, heads), norm_gain,
            )
        )
    )


def solution(mesh):
    n, nz = mesh.shape["seq"], mesh.shape["tp"]
    return jax.shard_map(
        functools.partial(on_device, n, nz),
        mesh=mesh,
        in_specs=(
            P(None, "seq", None), P(None, "tp"), P(None, "tp"), P(None, "tp"), P(None, "tp"),
            P(None, "tp"), P(), P("tp"), P("tp"), P("tp"),
        ),
        out_specs=P(None, "seq", "tp"),
        check_vma=False,
    )
```

```python
import functools
import math

import jax
import jax.numpy as jnp
from jax import lax
from jax.experimental import pallas as pl
from jax.experimental.pallas import tpu as pltpu
from jax.sharding import PartitionSpec as P

MESH = pl.DeviceIdType.MESH
F32, BF16 = jnp.float32, jnp.bfloat16
HEAD_DIM = 64
STATE = 128
CONV = 4
HALO = 16
CHUNK = 128
EPSILON = 1e-05
NN = (((1,), (0,)), ((), ()))
TN = (((0,), (0,)), ((), ()))
NT = (((1,), (1,)), ((), ()))


def dot(a, b, dims=NN):
    return lax.dot_general(a, b, dims, preferred_element_type=F32)


def split2(x):
    high = x.astype(BF16)
    low = (x - high.astype(F32)).astype(BF16)
    return jnp.concatenate([high, low], axis=0)


def bulk(view, send_sem, recv_sem, device_id):
    return pltpu.make_async_remote_copy(
        src_ref=view,
        dst_ref=view,
        send_sem=send_sem,
        recv_sem=recv_sem,
        device_id=device_id,
        device_id_type=MESH,
    )


def silu(x):
    half = 0.5 * x
    return half * jnp.tanh(half) + half


def conv_silu(window, taps, rows):
    total = taps[0:1] * window[5 : 5 + rows]
    for k in range(1, CONV):
        total = total + taps[k : k + 1] * window[5 + k : 5 + k + rows]
    return silu(total)


def kernel(
    n, nz, batch, length, inner, heads,
    hid_in, gate_in, value_in, bc_in, step_in, vconv_in, bconv_in, bias_in, rate_in, gain_in,
    out,
    vconv, bconv, bias, rate, gain, hid, wcat, stw, wsm, pre, xp, lhs, tbuf, bct, bcall, edget, edgeall, brows, crows, dsend, dall, dexp,
    sbuf, rbuf, pbuf, qbuf, sssend, ssall, rowx, e1t, e2t,
    load_sem, halo_s, halo_r, bc_s, bc_r, edge_s, edge_r, d_s, d_r, p_s, p_r, q_s, q_r, ss_s, ss_r,
):
    me = lax.axis_index("seq")
    z = lax.axis_index("tp")
    step_rows = length + HALO
    chunks = length // CHUNK
    piece = batch * STATE // n
    per_batch = n // batch
    nbc = bct.shape[1]
    half = nz // 2
    next_seq, next_tp = {"seq": lax.rem(me + 1, n)}, {"tp": lax.rem(z + 1, nz)}
    width = hid.shape[1]

    loads = []
    for b in range(batch):
        loads.append(
            pltpu.make_async_copy(
                hid_in.at[b], hid.at[pl.ds(b * step_rows + HALO, length)], load_sem.at[b]
            )
        )
    loads.append(pltpu.make_async_copy(bc_in, wsm.at[pl.ds(0, nbc)], load_sem.at[2]))
    loads.append(pltpu.make_async_copy(step_in, stw, load_sem.at[3]))
    loads.append(pltpu.make_async_copy(value_in, wcat.at[:, pl.ds(0, inner)], load_sem.at[4]))
    loads.append(pltpu.make_async_copy(gate_in, wcat.at[:, pl.ds(inner, inner)], load_sem.at[5]))
    tables = ((vconv_in, vconv), (bconv_in, bconv), (bias_in, bias), (rate_in, rate), (gain_in, gain))
    for k, (source, target) in enumerate(tables):
        loads.append(pltpu.make_async_copy(source, target, load_sem.at[6 + k]))
    for k in (2, 3, 0, 1, 8, 9, 7, 6, 10):
        loads[k].start()

    barrier = pltpu.get_barrier_semaphore()

    def greet_seq(d, carry):
        pl.semaphore_signal(
            barrier, inc=1, device_id={"seq": lax.rem(me + d, n)}, device_id_type=MESH
        )
        return carry

    def greet_tp(d, carry):
        pl.semaphore_signal(
            barrier, inc=1, device_id={"tp": lax.rem(z + d, nz)}, device_id_type=MESH
        )
        return carry

    lax.fori_loop(1, n, greet_seq, 0)
    lax.fori_loop(1, nz, greet_tp, 0)

    head_of = lax.broadcasted_iota(jnp.int32, (16, inner), 1) // HEAD_DIM
    spread16 = (head_of == lax.broadcasted_iota(jnp.int32, (16, inner), 0)).astype(F32)
    spread = jnp.concatenate([spread16, spread16], axis=0).astype(BF16)
    upper = (
        lax.broadcasted_iota(jnp.int32, (length, length), 0)
        <= lax.broadcasted_iota(jnp.int32, (length, length), 1)
    ).astype(F32).astype(BF16)

    loads[2].wait()
    loads[3].wait()
    wsm[nbc : nbc + heads, :] = stw[...]
    wsm[nbc + heads : nbc + 16, :] = jnp.zeros((16 - heads, width), BF16)

    raws = []

    def project_small(b):
        loads[b].wait()
        if b == 0:
            loads[4].start()
            loads[5].start()
        rows = pl.ds(b * step_rows + HALO, length)
        both = jnp.transpose(dot(hid[rows, :], wsm[...], NT))
        bct[b] = both[0:nbc].astype(BF16)
        raws.append(both[nbc : nbc + 16])

    project_small(0)
    pl.semaphore_wait(barrier, n - 1 + nz - 1)

    def halo_copy(b, target):
        return pltpu.make_async_remote_copy(
            src_ref=hid_in.at[b, pl.ds(length - HALO, HALO)],
            dst_ref=hid.at[pl.ds(b * step_rows, HALO)],
            send_sem=halo_s.at[b],
            recv_sem=halo_r.at[b],
            device_id={"seq": target},
            device_id_type=MESH,
        )

    following = lax.rem(me + 1, n)

    @pl.when(me < n - 1)
    def _():
        for b in range(batch):
            halo_copy(b, following).start()

    @pl.when(me == 0)
    def _():
        for b in range(batch):
            hid[pl.ds(b * step_rows, HALO), :] = jnp.zeros((HALO, width), BF16)

    relayed = nz == 8

    def bc_copy(source, target, b, held=None):
        return pltpu.make_async_remote_copy(
            src_ref=bct.at[b] if held is None else held,
            dst_ref=bcall.at[source, b],
            send_sem=bc_s,
            recv_sem=bc_r.at[b, source],
            device_id={"tp": target},
            device_id_type=MESH,
        )

    def send_bc(b):
        def bc_start(d, carry):
            bc_copy(z, lax.rem(z + d, nz), b).start()
            return carry

        if relayed:
            for d in (2, nz - 2, 1, nz - 1):
                bc_start(d, 0)
        else:
            lax.fori_loop(1, nz, bc_start, 0)
        bcall[z, b] = bct[b]

    def relay_bc(b):
        for d in (2, nz - 2):
            source = lax.rem(z + d, nz)
            bc_copy(source, z, b).wait_recv()
            back = 1 if d == nz - 2 else nz - 1
            hops = (2 * back, back) if (b == 0) == (back == 1) else (back,)
            for hop in hops:
                bc_copy(source, lax.rem(z + hop, nz), b, bcall.at[source, b]).start()

    send_bc(0)

    for b in range(1, batch):
        project_small(b)
        send_bc(b)

    loads[8].wait()
    loads[9].wait()
    table = jnp.concatenate([bias[...], rate[...], jnp.zeros((6, heads), F32)], axis=0)
    table = jnp.concatenate([table, jnp.zeros((8, 128 - heads), F32)], axis=1)
    columns = jnp.transpose(table)
    bias_col, rate_col = columns[0:16, 0:1], jnp.exp(columns[0:16, 1:2])
    live = lax.broadcasted_iota(jnp.int32, (16, length), 0) < heads
    steps, parts = [], []
    for b in range(batch):
        raw = jnp.where(live, raws[b] + bias_col, 0.0)
        size = jnp.maximum(raw, 0.0) + jnp.log1p(jnp.exp(-jnp.abs(raw)))
        size = jnp.where(live, size, 0.0)
        steps.append(size)
        parts.append(split2(-size * rate_col))
    summed = dot(jnp.concatenate(parts, axis=0), upper)
    lane = lax.broadcasted_iota(jnp.int32, (16, 128), 1)
    factors = jnp.zeros((16, 128), F32)
    for b in range(batch):
        cum = summed[32 * b : 32 * b + 16] + summed[32 * b + 16 : 32 * b + 32]
        begin = jnp.zeros((16, 1), F32)
        for c in range(chunks):
            here = cum[:, c * CHUNK : (c + 1) * CHUNK]
            end = here[:, CHUNK - 1 : CHUNK]
            ref = 0.5 * (begin + end)
            q = b * chunks + c
            e1t[q] = split2(jnp.exp(ref - here) * steps[b][:, c * CHUNK : (c + 1) * CHUNK])
            e2t[q] = split2(jnp.exp(here - ref))
            for kind, value in enumerate((ref - begin, end - begin, end - ref, ref)):
                factors = jnp.where(lane == kind * 8 + q, value, factors)
            begin = end
        factors = jnp.where(lane == 32 + b, begin, factors)
    factors = jnp.exp(factors)
    rowx[...] = dot(split2(factors), spread, TN)
    totals = jnp.transpose(factors)
    for b in range(batch):
        row = jnp.concatenate(
            [totals[32 + b : 33 + b], jnp.zeros((1, 112), F32)], axis=1
        )
        dsend[b] = jnp.broadcast_to(row, (8, 128))

    def d_copy(source, target):
        return pltpu.make_async_remote_copy(
            src_ref=dsend.at[target // per_batch],
            dst_ref=dall.at[source],
            send_sem=d_s,
            recv_sem=d_r,
            device_id={"seq": target},
            device_id_type=MESH,
        )

    def d_start(d, carry):
        d_copy(me, lax.rem(me + d, n)).start()
        return carry

    lax.fori_loop(1, n, d_start, 0)
    dall[me] = dsend[me // per_batch]


    loads[5].wait()
    tiles = 2 * inner // 256
    value_tiles = -(-inner // 256)

    def project_gate(t, carry):
        columns_at = pl.ds(pl.multiple_of(t * 256, 256), 256)
        for b in range(batch):
            rows = pl.ds(b * step_rows + HALO, length)
            pre[rows, columns_at] = dot(hid[rows, :], wcat[:, columns_at])
        return carry

    @pl.when(me > 0)
    def _():
        for b in range(batch):
            halo_copy(b, following).wait_recv()

    edge = dot(
        wsm[0:nbc, :],
        jnp.concatenate([hid[pl.ds(b * step_rows, HALO), :] for b in range(batch)], axis=0),
        NT,
    )
    edge = jnp.concatenate([edge, jnp.zeros((nbc, 128 - batch * HALO), F32)], axis=1)
    edget[...] = edge.astype(BF16)
    edgeall[z] = edge.astype(BF16)

    def edge_copy(source, target):
        return pltpu.make_async_remote_copy(
            src_ref=edget,
            dst_ref=edgeall.at[source],
            send_sem=edge_s,
            recv_sem=edge_r,
            device_id={"tp": target},
            device_id_type=MESH,
        )

    def edge_start(d, carry):
        edge_copy(z, lax.rem(z + d, nz)).start()
        return carry

    lax.fori_loop(1, nz, edge_start, 0)

    loads[4].wait()

    def project(t, carry):
        columns_at = pl.ds(pl.multiple_of(t * 256, 256), 256)
        for half in range(batch):
            rows = pl.ds(half * step_rows, step_rows)
            pre[rows, columns_at] = (
                dot(hid[rows, :], wcat[:, columns_at]).astype(BF16).astype(F32)
            )
        return carry

    if relayed:
        relay_bc(0)
        lax.fori_loop(0, 1, project, 0)
        relay_bc(1)
        lax.fori_loop(1, value_tiles, project, 0)
    else:
        lax.fori_loop(0, value_tiles, project, 0)

    loads[6].wait()
    vtaps = vconv[...]

    def values_of(q, carry):
        base = pl.multiple_of((q // chunks) * step_rows + lax.rem(q, chunks) * CHUNK + 8, 8)
        scale = dot(e1t[q], spread, TN)
        for col in range(0, inner, 128):
            cols = slice(col, col + 128)
            rows = conv_silu(pre[pl.ds(base, CHUNK + 8), cols], vtaps[:, cols], CHUNK)
            xp[q, :, cols] = (rows * scale[:, cols]).astype(BF16)
        return carry

    lax.fori_loop(0, batch * chunks, values_of, 0)

    def bc_wait(group):
        for s in range(group * half, (group + 1) * half):
            away = lax.rem(s + nz - z, nz)
            missing = away != 0
            if relayed:
                missing &= (away != 2) & (away != nz - 2)

            @pl.when(missing)
            def _(s=s):
                for b in range(batch):
                    bc_copy(s, z, b).wait_recv()

    loads[7].wait()
    taps = jnp.transpose(
        jnp.concatenate([bconv[...], jnp.zeros((8 - CONV, 2 * STATE), F32)], axis=0)
    )

    def conv_rows(first, b):
        sources = slice(first * half, (first + 1) * half)
        tail = edgeall[sources].reshape(STATE, 128).astype(F32)
        tail = pltpu.roll(tail, 128 - (b + 1) * HALO, 1)
        body = bcall[sources, b].reshape(STATE, length).astype(F32)
        whole = jnp.concatenate([tail, body], axis=1)
        weights = taps[first * STATE : (first + 1) * STATE]
        total = weights[:, CONV - 1 : CONV] * body
        for k in range(CONV - 1):
            shifted = pltpu.roll(whole, CONV - 1 - k, 1)[:, 128:]
            total = total + weights[:, k : k + 1] * shifted
        return silu(total).astype(BF16)

    bc_wait(0)
    bulk(edgeall.at[pl.ds(0, nz - 1)], edge_s, edge_r, next_tp).wait_recv()

    for b in range(batch):
        brows[:, b * length : (b + 1) * length] = conv_rows(0, b)

    causal = (
        lax.broadcasted_iota(jnp.int32, (CHUNK, CHUNK), 0)
        >= lax.broadcasted_iota(jnp.int32, (CHUNK, CHUNK), 1)
    )
    for b in range(batch):
        state = jnp.zeros((STATE, inner), F32)
        for c in range(chunks):
            q = b * chunks + c
            lanes = slice(b * length + c * CHUNK, b * length + (c + 1) * CHUNK)
            rows = brows[:, lanes]
            if c:
                tbuf[q] = (state * rowx[q : q + 1]).astype(BF16)
                state = state * rowx[8 + q : 9 + q]
            else:
                tbuf[q] = jnp.zeros((STATE, inner), BF16)
            state = state + rowx[16 + q : 17 + q] * dot(rows, xp[q])
        sbuf[b * per_batch : (b + 1) * per_batch] = state.reshape(
            per_batch, piece, inner
        ).astype(BF16)
    rbuf[me] = sbuf[me]

    def p_copy(source, target):
        return pltpu.make_async_remote_copy(
            src_ref=sbuf.at[target],
            dst_ref=rbuf.at[source],
            send_sem=p_s,
            recv_sem=p_r,
            device_id={"seq": target},
            device_id_type=MESH,
        )

    def p_start(d, carry):
        p_copy(me, lax.rem(me + d, n)).start()
        return carry

    lax.fori_loop(1, n, p_start, 0)

    lax.fori_loop(value_tiles, tiles, project_gate, 0)

    bulk(dall.at[pl.ds(0, n - 1)], d_s, d_r, next_seq).wait_recv()
    decays = dall[...].reshape(n * 8, 128)[:, 0:16]
    high = decays.astype(BF16)
    low = (decays - high.astype(F32)).astype(BF16)
    dexp[...] = (dot(high, spread[0:16]) + dot(low, spread[0:16])).reshape(n, 8, inner)

    bc_wait(1)
    for b in range(batch):
        crows[:, b * length : (b + 1) * length] = conv_rows(1, b)
    for q in range(batch * chunks):
        lanes = slice(q * CHUNK, (q + 1) * CHUNK)
        b_t = brows[:, lanes]
        c_t = crows[:, lanes]
        scores = dot(c_t, b_t, TN)
        lhs[q, :, 0:CHUNK] = jnp.where(causal, scores, 0.0).astype(BF16)
        lhs[q, :, CHUNK:] = jnp.transpose(c_t.astype(F32)).astype(BF16)

    bulk(rbuf.at[pl.ds(0, n - 1)], p_s, p_r, next_seq).wait_recv()

    def scan_step(i, prefix):
        pbuf[i] = prefix.astype(BF16)
        return dexp[i, 0:1, :] * prefix + rbuf[i].astype(F32)

    lax.fori_loop(0, n, scan_step, jnp.zeros((piece, inner), F32))

    def q_copy(source, target):
        return pltpu.make_async_remote_copy(
            src_ref=pbuf.at[target],
            dst_ref=qbuf.at[source],
            send_sem=q_s,
            recv_sem=q_r,
            device_id={"seq": target},
            device_id_type=MESH,
        )

    def q_start(d, carry):
        q_copy(me, lax.rem(me + d, n)).start()
        return carry

    lax.fori_loop(1, n, q_start, 0)
    qbuf[me] = pbuf[me]

    def local_of(q, carry):
        base = pl.multiple_of((q // chunks) * step_rows + lax.rem(q, chunks) * CHUNK + HALO, 8)
        at = pl.ds(base, CHUNK)
        scale = dot(e2t[q], spread, TN)
        mixed = dot(lhs[q], jnp.concatenate([xp[q], tbuf[q]], axis=0))
        which = lax.broadcasted_iota(jnp.int32, (8, inner), 0) == q
        refs = jnp.sum(jnp.where(which, rowx[24:32, :], 0.0), axis=0, keepdims=True)
        for col in range(0, inner, 128):
            cols = slice(inner + col, inner + col + 128)
            gate = silu(pre[at, cols]) * scale[:, col : col + 128]
            pre[at, col : col + 128] = mixed[:, col : col + 128] * gate
            pre[at, cols] = gate * refs[:, col : col + 128]
        return carry

    lax.fori_loop(0, batch * chunks, local_of, 0)

    bulk(dall.at[pl.ds(0, n - 1)], d_s, d_r, next_seq).wait_send()
    bulk(rbuf.at[pl.ds(0, n - 1)], p_s, p_r, next_seq).wait_send()

    bulk(qbuf.at[pl.ds(0, n - 1)], q_s, q_r, next_seq).wait_recv()

    picked = lax.broadcasted_iota(jnp.int32, (8, CHUNK), 0)
    squares = jnp.zeros((8, CHUNK), F32)
    loads[10].wait()
    gains = gain[...].reshape(1, inner)
    for b in range(batch):
        entering = qbuf[b * per_batch : (b + 1) * per_batch].astype(F32)
        entering = entering.reshape(STATE, inner).astype(BF16)
        at = pl.ds(b * step_rows + HALO, length)
        readout = lhs[b * chunks : (b + 1) * chunks, :, CHUNK:].reshape(length, STATE)
        sums = jnp.zeros((8, length), F32)
        for col in range(0, inner, 256):
            last = min(col + 256, inner)
            gated = pre[at, col:last] + dot(readout, entering[:, col:last]) * pre[
                at, inner + col : inner + last
            ]
            pre[at, col:last] = gated * gains[:, col:last]
            sums += dot(jnp.ones((8, last - col), BF16), (gated * gated).astype(BF16), NT)
        for c in range(chunks):
            part = sums[:, c * CHUNK : (c + 1) * CHUNK]
            squares = jnp.where(picked == b * chunks + c, part, squares)
    sssend[...] = squares

    def ss_copy(source, target):
        return pltpu.make_async_remote_copy(
            src_ref=sssend,
            dst_ref=ssall.at[source],
            send_sem=ss_s,
            recv_sem=ss_r,
            device_id={"tp": target},
            device_id_type=MESH,
        )

    def ss_start(d, carry):
        ss_copy(z, lax.rem(z + d, nz)).start()
        return carry

    lax.fori_loop(1, nz, ss_start, 0)
    ssall[z] = squares

    @pl.when(me < n - 1)
    def _():
        for b in range(batch):
            halo_copy(b, following).wait_send()

    bulk(qbuf.at[pl.ds(0, n - 1)], q_s, q_r, next_seq).wait_send()
    bulk(bcall.at[pl.ds(0, nz - 1)], bc_s, bc_r.at[0, 0], next_tp).wait_send()
    bulk(edgeall.at[pl.ds(0, nz - 1)], edge_s, edge_r, next_tp).wait_send()

    bulk(ssall.at[pl.ds(0, nz - 1)], ss_s, ss_r, next_tp).wait_recv()

    whole = ssall[0]
    for s in range(1, nz):
        whole = whole + ssall[s]
    factor = lax.rsqrt(whole / (inner * nz) + EPSILON)
    wide = jnp.ones((16, 128), BF16)

    for b in range(batch):
        for c in range(chunks):
            q = b * chunks + c
            mine = split2(jnp.where(picked == q, factor, 0.0))
            scale = dot(mine, wide, TN)
            at = pl.ds(b * step_rows + HALO + c * CHUNK, CHUNK)
            for col in range(0, inner, 128):
                out[b, c * CHUNK : (c + 1) * CHUNK, col : col + 128] = (
                    pre[at, col : col + 128] * scale
                ).astype(BF16)

    bulk(ssall.at[pl.ds(0, nz - 1)], ss_s, ss_r, next_tp).wait_send()


def on_device(
    n, nz, hidden_in, gate_proj, value_proj, bc_proj, step_proj,
    value_conv, bc_conv, step_bias, log_rate, norm_gain,
):
    batch, length, width = hidden_in.shape
    inner, heads, nbc = value_proj.shape[1], step_proj.shape[1], bc_proj.shape[1]
    chunks = batch * length // CHUNK
    rows = batch * (length + HALO)
    piece = batch * STATE // n
    hbm = pl.BlockSpec(memory_space=pltpu.HBM)
    dma = pltpu.SemaphoreType.DMA
    return pl.pallas_call(
        functools.partial(kernel, n, nz, batch, length, inner, heads),
        out_shape=jax.ShapeDtypeStruct((batch, length, inner), BF16),
        in_specs=[hbm] * 10,
        out_specs=pl.BlockSpec(memory_space=pltpu.VMEM),
        scratch_shapes=[
            pltpu.VMEM(value_conv.shape, F32),
            pltpu.VMEM(bc_conv.shape, F32),
            pltpu.VMEM((1, heads), F32),
            pltpu.VMEM((1, heads), F32),
            pltpu.VMEM((inner,), F32),
            pltpu.VMEM((rows, width), BF16),
            pltpu.VMEM((width, 2 * inner), BF16),
            pltpu.VMEM((heads, width), BF16),
            pltpu.VMEM((nbc + 16, width), BF16),
            pltpu.VMEM((rows, 2 * inner), F32),
            pltpu.VMEM((chunks, CHUNK, inner), BF16),
            pltpu.VMEM((chunks, CHUNK, CHUNK + STATE), BF16),
            pltpu.VMEM((chunks, STATE, inner), BF16),
            pltpu.VMEM((batch, nbc, length), BF16),
            pltpu.VMEM((nz, batch, nbc, length), BF16),
            pltpu.VMEM((nbc, 128), BF16),
            pltpu.VMEM((nz, nbc, 128), BF16),
            pltpu.VMEM((STATE, batch * length), BF16),
            pltpu.VMEM((STATE, batch * length), BF16),
            pltpu.VMEM((batch, 8, 128), F32),
            pltpu.VMEM((n, 8, 128), F32),
            pltpu.VMEM((n, 8, inner), F32),
            pltpu.VMEM((n, piece, inner), BF16),
            pltpu.VMEM((n, piece, inner), BF16),
            pltpu.VMEM((n, piece, inner), BF16),
            pltpu.VMEM((n, piece, inner), BF16),
            pltpu.VMEM((8, CHUNK), F32),
            pltpu.VMEM((nz, 8, CHUNK), F32),
            pltpu.VMEM((128, inner), F32),
            pltpu.VMEM((chunks, 32, CHUNK), BF16),
            pltpu.VMEM((chunks, 32, CHUNK), BF16),
            dma((11,)),
            dma((batch,)), dma((batch,)),
            dma, dma((batch, nz)),
            dma, dma,
            dma, dma,
            dma, dma,
            dma, dma,
            dma, dma,
        ],
        compiler_params=pltpu.CompilerParams(
            collective_id=0, has_side_effects=True, vmem_limit_bytes=52 * 1024 * 1024
        ),
    )(
        *(
            pltpu.with_memory_space_constraint(x, pltpu.HBM)
            for x in (
                hidden_in, gate_proj, value_proj, bc_proj.T, step_proj.T, value_conv, bc_conv,
                step_bias.reshape(1, heads), log_rate.reshape(1, heads), norm_gain,
            )
        )
    )


def solution(mesh):
    n, nz = mesh.shape["seq"], mesh.shape["tp"]
    return jax.shard_map(
        functools.partial(on_device, n, nz),
        mesh=mesh,
        in_specs=(
            P(None, "seq", None), P(None, "tp"), P(None, "tp"), P(None, "tp"), P(None, "tp"),
            P(None, "tp"), P(), P("tp"), P("tp"), P("tp"),
        ),
        out_specs=P(None, "seq", "tp"),
        check_vma=False,
    )
```

```python
import functools
import math

import jax
import jax.numpy as jnp
from jax import lax
from jax.experimental import pallas as pl
from jax.experimental.pallas import tpu as pltpu
from jax.sharding import PartitionSpec as P

MESH = pl.DeviceIdType.MESH
F32, BF16 = jnp.float32, jnp.bfloat16
HEAD_DIM = 64
STATE = 128
CONV = 4
HALO = 16
CHUNK = 128
EPSILON = 1e-05
NN = (((1,), (0,)), ((), ()))
TN = (((0,), (0,)), ((), ()))
NT = (((1,), (1,)), ((), ()))


def dot(a, b, dims=NN):
    return lax.dot_general(a, b, dims, preferred_element_type=F32)


def split2(x):
    high = x.astype(BF16)
    low = (x - high.astype(F32)).astype(BF16)
    return jnp.concatenate([high, low], axis=0)


def bulk(view, send_sem, recv_sem, device_id):
    return pltpu.make_async_remote_copy(
        src_ref=view,
        dst_ref=view,
        send_sem=send_sem,
        recv_sem=recv_sem,
        device_id=device_id,
        device_id_type=MESH,
    )


def silu(x):
    half = 0.5 * x
    return half * jnp.tanh(half) + half


def conv_silu(window, taps, rows):
    total = taps[0:1] * window[5 : 5 + rows]
    for k in range(1, CONV):
        total = total + taps[k : k + 1] * window[5 + k : 5 + k + rows]
    return silu(total)


def kernel(
    n, nz, batch, length, inner, heads,
    hid_in, gate_in, value_in, bc_in, step_in, vconv_in, bconv_in, bias_in, rate_in, gain_in,
    out,
    vconv, bconv, bias, rate, gain, hid, wcat, stw, wsm, pre, xp, lhs, tbuf, bct, bcall, edget, edgeall, brows, crows, dsend, dall, dexp,
    sbuf, rbuf, pbuf, qbuf, sssend, ssall, rowx, e1t, e2t,
    load_sem, halo_s, halo_r, bc_s, bc_r, edge_s, edge_r, d_s, d_r, p_s, p_r, q_s, q_r, ss_s, ss_r,
):
    me = lax.axis_index("seq")
    z = lax.axis_index("tp")
    step_rows = length + HALO
    chunks = length // CHUNK
    piece = batch * STATE // n
    per_batch = n // batch
    nbc = bct.shape[1]
    half = nz // 2

    next_seq, next_tp = {"seq": lax.rem(me + 1, n)}, {"tp": lax.rem(z + 1, nz)}
    width = hid.shape[1]

    loads = []
    for b in range(batch):
        loads.append(
            pltpu.make_async_copy(
                hid_in.at[b], hid.at[pl.ds(b * step_rows + HALO, length)], load_sem.at[b]
            )
        )
    loads.append(pltpu.make_async_copy(bc_in, wsm.at[pl.ds(0, nbc)], load_sem.at[2]))
    loads.append(pltpu.make_async_copy(step_in, stw, load_sem.at[3]))
    loads.append(pltpu.make_async_copy(value_in, wcat.at[:, pl.ds(0, inner)], load_sem.at[4]))
    loads.append(pltpu.make_async_copy(gate_in, wcat.at[:, pl.ds(inner, inner)], load_sem.at[5]))
    tables = ((vconv_in, vconv), (bconv_in, bconv), (bias_in, bias), (rate_in, rate), (gain_in, gain))
    for k, (source, target) in enumerate(tables):
        loads.append(pltpu.make_async_copy(source, target, load_sem.at[6 + k]))
    for k in (2, 3, 0, 1, 8, 9, 7, 6, 10):
        loads[k].start()

    barrier = pltpu.get_barrier_semaphore()

    def greet_seq(d, carry):
        pl.semaphore_signal(
            barrier, inc=1, device_id={"seq": lax.rem(me + d, n)}, device_id_type=MESH
        )
        return carry

    def greet_tp(d, carry):
        pl.semaphore_signal(
            barrier, inc=1, device_id={"tp": lax.rem(z + d, nz)}, device_id_type=MESH
        )
        return carry

    lax.fori_loop(1, n, greet_seq, 0)
    lax.fori_loop(1, nz, greet_tp, 0)

    head_of = lax.broadcasted_iota(jnp.int32, (16, inner), 1) // HEAD_DIM
    spread16 = (head_of == lax.broadcasted_iota(jnp.int32, (16, inner), 0)).astype(F32)
    spread = jnp.concatenate([spread16, spread16], axis=0).astype(BF16)
    upper = (
        lax.broadcasted_iota(jnp.int32, (length, length), 0)
        <= lax.broadcasted_iota(jnp.int32, (length, length), 1)
    ).astype(F32).astype(BF16)

    loads[2].wait()
    loads[3].wait()
    wsm[nbc : nbc + heads, :] = stw[...]
    wsm[nbc + heads : nbc + 16, :] = jnp.zeros((16 - heads, width), BF16)

    raws = []

    def project_small(b):
        loads[b].wait()
        if b == 0:
            loads[4].start()
            loads[5].start()
        rows = pl.ds(b * step_rows + HALO, length)
        both = jnp.transpose(dot(hid[rows, :], wsm[...], NT))
        bct[b] = both[0:nbc].astype(BF16)
        raws.append(both[nbc : nbc + 16])

    project_small(0)
    pl.semaphore_wait(barrier, n - 1 + nz - 1)

    def halo_copy(b, target):
        return pltpu.make_async_remote_copy(
            src_ref=hid_in.at[b, pl.ds(length - HALO, HALO)],
            dst_ref=hid.at[pl.ds(b * step_rows, HALO)],
            send_sem=halo_s.at[b],
            recv_sem=halo_r.at[b],
            device_id={"seq": target},
            device_id_type=MESH,
        )

    following = lax.rem(me + 1, n)

    @pl.when(me < n - 1)
    def _():
        for b in range(batch):
            halo_copy(b, following).start()

    @pl.when(me == 0)
    def _():
        for b in range(batch):
            hid[pl.ds(b * step_rows, HALO), :] = jnp.zeros((HALO, width), BF16)

    relayed = nz == 8

    def bc_copy(source, target, b, held=None):
        return pltpu.make_async_remote_copy(
            src_ref=bct.at[b] if held is None else held,
            dst_ref=bcall.at[source, b],
            send_sem=bc_s,
            recv_sem=bc_r.at[b, source],
            device_id={"tp": target},
            device_id_type=MESH,
        )

    def send_bc(b):
        def bc_start(d, carry):
            bc_copy(z, lax.rem(z + d, nz), b).start()
            return carry

        if relayed:
            for d in (2, nz - 2, 1, nz - 1):
                bc_start(d, 0)
        else:
            lax.fori_loop(1, nz, bc_start, 0)
        bcall[z, b] = bct[b]

    def relay_bc(b):
        for d in (2, nz - 2):
            source = lax.rem(z + d, nz)
            bc_copy(source, z, b).wait_recv()
            back = 1 if d == nz - 2 else nz - 1
            hops = (2 * back, back) if (b == 0) == (back == 1) else (back,)
            for hop in hops:
                bc_copy(source, lax.rem(z + hop, nz), b, bcall.at[source, b]).start()

    send_bc(0)

    for b in range(1, batch):
        project_small(b)
        send_bc(b)

    loads[8].wait()
    loads[9].wait()
    table = jnp.concatenate([bias[...], rate[...], jnp.zeros((6, heads), F32)], axis=0)
    table = jnp.concatenate([table, jnp.zeros((8, 128 - heads), F32)], axis=1)
    columns = jnp.transpose(table)
    bias_col, rate_col = columns[0:16, 0:1], jnp.exp(columns[0:16, 1:2])
    live = lax.broadcasted_iota(jnp.int32, (16, length), 0) < heads
    steps, parts = [], []
    for b in range(batch):
        raw = jnp.where(live, raws[b] + bias_col, 0.0)
        size = jnp.maximum(raw, 0.0) + jnp.log1p(jnp.exp(-jnp.abs(raw)))
        size = jnp.where(live, size, 0.0)
        steps.append(size)
        parts.append(split2(-size * rate_col))
    summed = dot(jnp.concatenate(parts, axis=0), upper)
    lane = lax.broadcasted_iota(jnp.int32, (16, 128), 1)
    factors = jnp.zeros((16, 128), F32)
    for b in range(batch):
        cum = summed[32 * b : 32 * b + 16] + summed[32 * b + 16 : 32 * b + 32]
        begin = jnp.zeros((16, 1), F32)
        for c in range(chunks):
            here = cum[:, c * CHUNK : (c + 1) * CHUNK]
            end = here[:, CHUNK - 1 : CHUNK]
            ref = 0.5 * (begin + end)
            q = b * chunks + c
            e1t[q] = split2(jnp.exp(ref - here) * steps[b][:, c * CHUNK : (c + 1) * CHUNK])
            e2t[q] = split2(jnp.exp(here - ref))
            for kind, value in enumerate((ref - begin, end - begin, end - ref, ref)):
                factors = jnp.where(lane == kind * 8 + q, value, factors)
            begin = end
        factors = jnp.where(lane == 32 + b, begin, factors)
    factors = jnp.exp(factors)
    rowx[...] = dot(split2(factors), spread, TN)
    totals = jnp.transpose(factors)
    for b in range(batch):
        row = jnp.concatenate(
            [totals[32 + b : 33 + b], jnp.zeros((1, 112), F32)], axis=1
        )
        dsend[b] = jnp.broadcast_to(row, (8, 128))

    def d_copy(source, target):
        return pltpu.make_async_remote_copy(
            src_ref=dsend.at[target // per_batch],
            dst_ref=dall.at[source],
            send_sem=d_s,
            recv_sem=d_r,
            device_id={"seq": target},
            device_id_type=MESH,
        )

    def d_start(d, carry):
        d_copy(me, lax.rem(me + d, n)).start()
        return carry

    lax.fori_loop(1, n, d_start, 0)
    dall[me] = dsend[me // per_batch]


    loads[5].wait()
    tiles = 2 * inner // 256
    value_tiles = -(-inner // 256)

    def project_gate(t, carry):
        columns_at = pl.ds(pl.multiple_of(t * 256, 256), 256)
        for b in range(batch):
            rows = pl.ds(b * step_rows + HALO, length)
            pre[rows, columns_at] = dot(hid[rows, :], wcat[:, columns_at])
        return carry

    @pl.when(me > 0)
    def _():
        for b in range(batch):
            halo_copy(b, following).wait_recv()

    edge = dot(
        wsm[0:nbc, :],
        jnp.concatenate([hid[pl.ds(b * step_rows, HALO), :] for b in range(batch)], axis=0),
        NT,
    )
    edge = jnp.concatenate([edge, jnp.zeros((nbc, 128 - batch * HALO), F32)], axis=1)
    edget[...] = edge.astype(BF16)
    edgeall[z] = edge.astype(BF16)

    def edge_copy(source, target):
        return pltpu.make_async_remote_copy(
            src_ref=edget,
            dst_ref=edgeall.at[source],
            send_sem=edge_s,
            recv_sem=edge_r,
            device_id={"tp": target},
            device_id_type=MESH,
        )

    def edge_start(d, carry):
        edge_copy(z, lax.rem(z + d, nz)).start()
        return carry

    lax.fori_loop(1, nz, edge_start, 0)

    loads[4].wait()

    def project(t, carry):
        columns_at = pl.ds(pl.multiple_of(t * 256, 256), 256)
        for half in range(batch):
            rows = pl.ds(half * step_rows, step_rows)
            pre[rows, columns_at] = (
                dot(hid[rows, :], wcat[:, columns_at]).astype(BF16).astype(F32)
            )
        return carry

    if relayed:
        relay_bc(0)
        lax.fori_loop(0, 1, project, 0)
        relay_bc(1)
        lax.fori_loop(1, value_tiles, project, 0)
    else:
        lax.fori_loop(0, value_tiles, project, 0)

    loads[6].wait()
    vtaps = vconv[...]

    def values_of(q, carry):
        base = pl.multiple_of((q // chunks) * step_rows + lax.rem(q, chunks) * CHUNK + 8, 8)
        rows = conv_silu(pre[pl.ds(base, CHUNK + 8), 0:inner], vtaps, CHUNK)
        xp[q] = (rows * dot(e1t[q], spread, TN)).astype(BF16)
        return carry

    lax.fori_loop(0, batch * chunks, values_of, 0)

    def bc_wait(group):
        for s in range(group * half, (group + 1) * half):
            away = lax.rem(s + nz - z, nz)
            missing = away != 0
            if relayed:
                missing &= (away != 2) & (away != nz - 2)

            @pl.when(missing)
            def _(s=s):
                for b in range(batch):
                    bc_copy(s, z, b).wait_recv()

    loads[7].wait()
    taps = jnp.transpose(
        jnp.concatenate([bconv[...], jnp.zeros((8 - CONV, 2 * STATE), F32)], axis=0)
    )

    def conv_rows(first, b):
        sources = slice(first * half, (first + 1) * half)
        tail = edgeall[sources].reshape(STATE, 128).astype(F32)
        tail = pltpu.roll(tail, 128 - (b + 1) * HALO, 1)
        body = bcall[sources, b].reshape(STATE, length).astype(F32)
        whole = jnp.concatenate([tail, body], axis=1)
        weights = taps[first * STATE : (first + 1) * STATE]
        total = weights[:, CONV - 1 : CONV] * body
        for k in range(CONV - 1):
            shifted = pltpu.roll(whole, CONV - 1 - k, 1)[:, 128:]
            total = total + weights[:, k : k + 1] * shifted
        return silu(total).astype(BF16)

    bc_wait(0)
    bulk(edgeall.at[pl.ds(0, nz - 1)], edge_s, edge_r, next_tp).wait_recv()

    for b in range(batch):
        brows[:, b * length : (b + 1) * length] = conv_rows(0, b)

    causal = (
        lax.broadcasted_iota(jnp.int32, (CHUNK, CHUNK), 0)
        >= lax.broadcasted_iota(jnp.int32, (CHUNK, CHUNK), 1)
    )
    for b in range(batch):
        state = jnp.zeros((STATE, inner), F32)
        for c in range(chunks):
            q = b * chunks + c
            lanes = slice(b * length + c * CHUNK, b * length + (c + 1) * CHUNK)
            rows = brows[:, lanes]
            if c:
                tbuf[q] = (state * rowx[q : q + 1]).astype(BF16)
                state = state * rowx[8 + q : 9 + q]
            else:
                tbuf[q] = jnp.zeros((STATE, inner), BF16)
            state = state + rowx[16 + q : 17 + q] * dot(rows, xp[q])
        sbuf[b * per_batch : (b + 1) * per_batch] = state.reshape(
            per_batch, piece, inner
        ).astype(BF16)
    rbuf[me] = sbuf[me]

    def p_copy(source, target):
        return pltpu.make_async_remote_copy(
            src_ref=sbuf.at[target],
            dst_ref=rbuf.at[source],
            send_sem=p_s,
            recv_sem=p_r,
            device_id={"seq": target},
            device_id_type=MESH,
        )

    def p_start(d, carry):
        p_copy(me, lax.rem(me + d, n)).start()
        return carry

    for d in range(1, n):
        p_start(d, 0)

    lax.fori_loop(value_tiles, tiles, project_gate, 0)

    bulk(dall.at[pl.ds(0, n - 1)], d_s, d_r, next_seq).wait_recv()
    decays = dall[...].reshape(n * 8, 128)[:, 0:16]
    high = decays.astype(BF16)
    low = (decays - high.astype(F32)).astype(BF16)
    dexp[...] = (dot(high, spread[0:16]) + dot(low, spread[0:16])).reshape(n, 8, inner)

    bc_wait(1)
    for b in range(batch):
        crows[:, b * length : (b + 1) * length] = conv_rows(1, b)
    for q in range(batch * chunks):
        lanes = slice(q * CHUNK, (q + 1) * CHUNK)
        b_t = brows[:, lanes]
        c_t = crows[:, lanes]
        scores = dot(c_t, b_t, TN)
        lhs[q, :, 0:CHUNK] = jnp.where(causal, scores, 0.0).astype(BF16)
        lhs[q, :, CHUNK:] = jnp.transpose(c_t.astype(F32)).astype(BF16)

    bulk(rbuf.at[pl.ds(0, n - 1)], p_s, p_r, next_seq).wait_recv()

    def scan_step(i, prefix):
        pbuf[i] = prefix.astype(BF16)
        return dexp[i, 0:1, :] * prefix + rbuf[i].astype(F32)

    lax.fori_loop(0, n, scan_step, jnp.zeros((piece, inner), F32))

    def q_copy(source, target):
        return pltpu.make_async_remote_copy(
            src_ref=pbuf.at[target],
            dst_ref=qbuf.at[source],
            send_sem=q_s,
            recv_sem=q_r,
            device_id={"seq": target},
            device_id_type=MESH,
        )

    def q_start(d, carry):
        q_copy(me, lax.rem(me + d, n)).start()
        return carry

    for d in range(1, n):
        q_start(d, 0)
    qbuf[me] = pbuf[me]

    def local_of(q, carry):
        base = pl.multiple_of((q // chunks) * step_rows + lax.rem(q, chunks) * CHUNK + HALO, 8)
        at = pl.ds(base, CHUNK)
        scale = dot(e2t[q], spread, TN)
        mixed = dot(lhs[q], jnp.concatenate([xp[q], tbuf[q]], axis=0))
        which = lax.broadcasted_iota(jnp.int32, (8, inner), 0) == q
        refs = jnp.sum(jnp.where(which, rowx[24:32, :], 0.0), axis=0, keepdims=True)
        for col in range(0, inner, 128):
            cols = slice(inner + col, inner + col + 128)
            gate = silu(pre[at, cols]) * scale[:, col : col + 128]
            pre[at, col : col + 128] = mixed[:, col : col + 128] * gate
            pre[at, cols] = gate * refs[:, col : col + 128]
        return carry

    lax.fori_loop(0, batch * chunks, local_of, 0)

    bulk(dall.at[pl.ds(0, n - 1)], d_s, d_r, next_seq).wait_send()
    bulk(rbuf.at[pl.ds(0, n - 1)], p_s, p_r, next_seq).wait_send()

    bulk(qbuf.at[pl.ds(0, n - 1)], q_s, q_r, next_seq).wait_recv()

    picked = lax.broadcasted_iota(jnp.int32, (8, CHUNK), 0)
    squares = jnp.zeros((8, CHUNK), F32)
    loads[10].wait()
    gains = gain[...].reshape(1, inner)
    for b in range(batch):
        entering = qbuf[b * per_batch : (b + 1) * per_batch].astype(F32)
        entering = entering.reshape(STATE, inner).astype(BF16)
        at = pl.ds(b * step_rows + HALO, length)
        readout = lhs[b * chunks : (b + 1) * chunks, :, CHUNK:].reshape(length, STATE)
        sums = jnp.zeros((8, length), F32)
        for col in range(0, inner, 256):
            last = min(col + 256, inner)
            gated = pre[at, col:last] + dot(readout, entering[:, col:last]) * pre[
                at, inner + col : inner + last
            ]
            pre[at, col:last] = gated * gains[:, col:last]
            sums += dot(jnp.ones((8, last - col), BF16), (gated * gated).astype(BF16), NT)
        for c in range(chunks):
            part = sums[:, c * CHUNK : (c + 1) * CHUNK]
            squares = jnp.where(picked == b * chunks + c, part, squares)
    sssend[...] = squares

    def ss_copy(source, target):
        return pltpu.make_async_remote_copy(
            src_ref=sssend,
            dst_ref=ssall.at[source],
            send_sem=ss_s,
            recv_sem=ss_r,
            device_id={"tp": target},
            device_id_type=MESH,
        )

    def ss_start(d, carry):
        ss_copy(z, lax.rem(z + d, nz)).start()
        return carry

    lax.fori_loop(1, nz, ss_start, 0)
    ssall[z] = squares

    @pl.when(me < n - 1)
    def _():
        for b in range(batch):
            halo_copy(b, following).wait_send()

    bulk(qbuf.at[pl.ds(0, n - 1)], q_s, q_r, next_seq).wait_send()
    bulk(bcall.at[pl.ds(0, nz - 1)], bc_s, bc_r.at[0, 0], next_tp).wait_send()
    bulk(edgeall.at[pl.ds(0, nz - 1)], edge_s, edge_r, next_tp).wait_send()

    bulk(ssall.at[pl.ds(0, nz - 1)], ss_s, ss_r, next_tp).wait_recv()

    whole = ssall[0]
    for s in range(1, nz):
        whole = whole + ssall[s]
    factor = lax.rsqrt(whole / (inner * nz) + EPSILON)
    wide = jnp.ones((16, 128), BF16)

    for b in range(batch):
        for c in range(chunks):
            q = b * chunks + c
            mine = split2(jnp.where(picked == q, factor, 0.0))
            scale = dot(mine, wide, TN)
            at = pl.ds(b * step_rows + HALO + c * CHUNK, CHUNK)
            for col in range(0, inner, 128):
                out[b, c * CHUNK : (c + 1) * CHUNK, col : col + 128] = (
                    pre[at, col : col + 128] * scale
                ).astype(BF16)

    bulk(ssall.at[pl.ds(0, nz - 1)], ss_s, ss_r, next_tp).wait_send()


def on_device(
    n, nz, hidden_in, gate_proj, value_proj, bc_proj, step_proj,
    value_conv, bc_conv, step_bias, log_rate, norm_gain,
):
    batch, length, width = hidden_in.shape
    inner, heads, nbc = value_proj.shape[1], step_proj.shape[1], bc_proj.shape[1]
    chunks = batch * length // CHUNK
    rows = batch * (length + HALO)
    piece = batch * STATE // n
    hbm = pl.BlockSpec(memory_space=pltpu.HBM)
    dma = pltpu.SemaphoreType.DMA
    return pl.pallas_call(
        functools.partial(kernel, n, nz, batch, length, inner, heads),
        out_shape=jax.ShapeDtypeStruct((batch, length, inner), BF16),
        in_specs=[hbm] * 10,
        out_specs=pl.BlockSpec(memory_space=pltpu.VMEM),
        scratch_shapes=[
            pltpu.VMEM(value_conv.shape, F32),
            pltpu.VMEM(bc_conv.shape, F32),
            pltpu.VMEM((1, heads), F32),
            pltpu.VMEM((1, heads), F32),
            pltpu.VMEM((inner,), F32),
            pltpu.VMEM((rows, width), BF16),
            pltpu.VMEM((width, 2 * inner), BF16),
            pltpu.VMEM((heads, width), BF16),
            pltpu.VMEM((nbc + 16, width), BF16),
            pltpu.VMEM((rows, 2 * inner), F32),
            pltpu.VMEM((chunks, CHUNK, inner), BF16),
            pltpu.VMEM((chunks, CHUNK, CHUNK + STATE), BF16),
            pltpu.VMEM((chunks, STATE, inner), BF16),
            pltpu.VMEM((batch, nbc, length), BF16),
            pltpu.VMEM((nz, batch, nbc, length), BF16),
            pltpu.VMEM((nbc, 128), BF16),
            pltpu.VMEM((nz, nbc, 128), BF16),
            pltpu.VMEM((STATE, batch * length), BF16),
            pltpu.VMEM((STATE, batch * length), BF16),
            pltpu.VMEM((batch, 8, 128), F32),
            pltpu.VMEM((n, 8, 128), F32),
            pltpu.VMEM((n, 8, inner), F32),
            pltpu.VMEM((n, piece, inner), BF16),
            pltpu.VMEM((n, piece, inner), BF16),
            pltpu.VMEM((n, piece, inner), BF16),
            pltpu.VMEM((n, piece, inner), BF16),
            pltpu.VMEM((8, CHUNK), F32),
            pltpu.VMEM((nz, 8, CHUNK), F32),
            pltpu.VMEM((128, inner), F32),
            pltpu.VMEM((chunks, 32, CHUNK), BF16),
            pltpu.VMEM((chunks, 32, CHUNK), BF16),
            dma((11,)),
            dma((batch,)), dma((batch,)),
            dma, dma((batch, nz)),
            dma, dma,
            dma, dma,
            dma, dma,
            dma, dma,
            dma, dma,
        ],
        compiler_params=pltpu.CompilerParams(
            collective_id=0, has_side_effects=True, vmem_limit_bytes=52 * 1024 * 1024
        ),
    )(
        *(
            pltpu.with_memory_space_constraint(x, pltpu.HBM)
            for x in (
                hidden_in, gate_proj, value_proj, bc_proj.T, step_proj.T, value_conv, bc_conv,
                step_bias.reshape(1, heads), log_rate.reshape(1, heads), norm_gain,
            )
        )
    )


def solution(mesh):
    n, nz = mesh.shape["seq"], mesh.shape["tp"]
    return jax.shard_map(
        functools.partial(on_device, n, nz),
        mesh=mesh,
        in_specs=(
            P(None, "seq", None), P(None, "tp"), P(None, "tp"), P(None, "tp"), P(None, "tp"),
            P(None, "tp"), P(), P("tp"), P("tp"), P("tp"),
        ),
        out_specs=P(None, "seq", "tp"),
        check_vma=False,
    )
```
